512 devices in a mesh: seq: 64 (over y, x, core), head: 8 (over z).
Axes of the slice: x: 4, y: 8, z: 8, core: 2. Of those that a mesh axis runs over, the one named last changes fastest.
Arguments:
- queries: bfloat16 [8192, 8192], P('seq', 'head'), may hold values from -6 to 6
- keys: bfloat16 [8192, 8192], P('seq', 'head'), may hold values from -6 to 6
- values: bfloat16 [8192, 8192], P('seq', 'head'), may hold values from -48 to 48, as said below
- cotangent: bfloat16 [8192, 8192], P('seq', 'head'), may hold values from -6 to 6
- gain: float32 [8192], P('head'), may hold values from 0.1 to 1.9
Outputs:
- query_grad: bfloat16 [8192, 8192], P('seq', 'head')
- key_grad: bfloat16 [8192, 8192], P('seq', 'head')
- value_grad: bfloat16 [8192, 8192], P('seq', 'head')
The draws below stay inside these ranges and needn't reach their ends.
Inputs may be any that keep to these rules, and one draw needn't show every extreme that they name: Real values.
All inputs are finite; a program needn't handle non-finite values.
Results may differ from the reference program's by a relative error of at most 0.0058.
Values sent between devices are 32-bit elements; how exact they have to be, the bound alone decides.
A program may use at most 128 MiB of HBM per device.

```python
import math
import jax
import jax.numpy as jnp
from jax import lax

HEADS = 64
HEAD_DIM = 128
T_DEV = 128
SEQ_LEN = 8192
WIDTH = 8192
N_SEQ = 64


def draw_values(key, part):
    first, second, third = jax.random.split(jax.random.fold_in(key, 17), 3)
    position = jnp.arange(WIDTH).astype(jnp.float32) / WIDTH
    column_scale = jnp.exp(math.log(3.0) * position) * jnp.exp(jax.random.uniform(second, (WIDTH,), jnp.float32, 0.0, math.log(4.0)))
    row_scale = jnp.exp(jax.random.uniform(third, (SEQ_LEN, 1), jnp.float32, 0.0, math.log(10.0)))
    base = jnp.clip(jax.random.normal(first, (SEQ_LEN, WIDTH), jnp.float32), -4.0, 4.0)
    return (0.1 * base * row_scale * column_scale[None, :]).astype(jnp.bfloat16)


def block_scale(stream_key, extent, shards, low, high):
    factor_of = 1.0
    for axis_at, blocks in shards:
        draws = jax.random.uniform(jax.random.fold_in(jax.random.fold_in(stream_key, 6), axis_at), (blocks,), jnp.float32, low / len(shards), high / len(shards))
        factor_of = factor_of * jnp.repeat(jnp.exp(draws), extent[axis_at] // blocks).reshape((-1,) + (1,) * (len(extent) - 1 - axis_at))
    return factor_of


def bell_draw(key, dims, spread, bound, cuts=(), kind=jnp.bfloat16):
    loudness = block_scale(key, dims, cuts, -0.22, 0.18) if cuts else 1.0
    drawn = jax.random.normal(key, dims, jnp.float32) * spread * loudness
    return jnp.minimum(jnp.maximum(drawn, -bound), bound).astype(kind)


def setup_inputs(seed: int = 0) -> dict:
    streams_of = jax.random.split(jax.random.key(seed), 6)
    queries = bell_draw(streams_of[0], (SEQ_LEN, WIDTH), 1.0, 6.0, ((0, 64), (1, 8)))
    keys = bell_draw(streams_of[1], (SEQ_LEN, WIDTH), 1.0, 6.0, ((0, 64), (1, 8)))
    values = draw_values(jax.random.fold_in(streams_of[5], 71), 0)
    cotangent = bell_draw(streams_of[3], (SEQ_LEN, WIDTH), 1.0, 6.0, ((0, 64), (1, 8)))
    gain = jnp.clip(1.0 + 0.18 * jax.random.normal(streams_of[4], (WIDTH,), jnp.float32), 0.1, 1.9)
    return dict(queries=queries, keys=keys, values=values, cotangent=cotangent, gain=gain)


epsilon = 1e-05

def split_blocks(array):
    return array.reshape(N_SEQ, T_DEV, HEADS, HEAD_DIM).astype(jnp.float32)

def reference(queries, keys, values, cotangent, gain):
    score_scale = HEAD_DIM ** (-0.5)
    rows_index = lax.broadcasted_iota(jnp.int32, (T_DEV, T_DEV), 0)
    cols_index = lax.broadcasted_iota(jnp.int32, (T_DEV, T_DEV), 1)
    causal_mask = (rows_index >= cols_index)[None, :, :]
    query_blocks = split_blocks(queries)
    key_blocks = split_blocks(keys)
    value_blocks = split_blocks(values)

    def block_weights(query_block, key_block):
        scores = jnp.einsum('thd,shd->hts', query_block, key_block) * score_scale
        rounded = jnp.where(causal_mask, scores, 0.0).astype(jnp.bfloat16)
        return lax.optimization_barrier(rounded).astype(jnp.float32)

    def forward_step(state, inputs):
        query_block, key_block, value_block = inputs
        state_low = lax.optimization_barrier(state.astype(jnp.bfloat16)).astype(jnp.float32)
        weights = block_weights(query_block, key_block)
        attended = jnp.einsum('hts,shd->thd', weights, value_block)
        attended = attended + score_scale * jnp.einsum('thd,hde->the', query_block, state_low)
        new_state = state + jnp.einsum('shd,she->hde', key_block, value_block)
        return (new_state, (attended, state_low))
    start_state = jnp.zeros((HEADS, HEAD_DIM, HEAD_DIM), jnp.float32)
    final_state, outputs = lax.scan(forward_step, start_state, (query_blocks, key_blocks, value_blocks))
    attended_blocks, prefix_blocks = outputs
    attended = attended_blocks.reshape(SEQ_LEN, WIDTH)
    squares = lax.optimization_barrier(jnp.mean(attended * attended, axis=1))
    inverse_rms = lax.rsqrt(squares + epsilon)
    normed = attended * inverse_rms[:, None]
    scaled = cotangent.astype(jnp.float32) * gain[None, :]
    cross = lax.optimization_barrier(jnp.mean(scaled * normed, axis=1))
    grad_attended = ((scaled - normed * cross[:, None]) * inverse_rms[:, None]).astype(jnp.bfloat16)
    grad_blocks = split_blocks(grad_attended)

    def backward_step(state, inputs):
        query_block, key_block, value_block, grad_block, prefix_low = inputs
        suffix_low = lax.optimization_barrier(state.astype(jnp.bfloat16)).astype(jnp.float32)
        weights = block_weights(query_block, key_block)
        grad_scores = jnp.einsum('the,she->hts', grad_block, value_block) * score_scale
        grad_weights = jnp.where(causal_mask, grad_scores, 0.0).astype(jnp.bfloat16)
        grad_weights = lax.optimization_barrier(grad_weights).astype(jnp.float32)
        query_grad = jnp.einsum('hts,shd->thd', grad_weights, key_block)
        query_grad = query_grad + score_scale * jnp.einsum('the,hde->thd', grad_block, prefix_low)
        key_grad = jnp.einsum('hts,thd->shd', grad_weights, query_block)
        key_grad = key_grad + score_scale * jnp.einsum('she,hde->shd', value_block, suffix_low)
        value_grad = jnp.einsum('hts,the->she', weights, grad_block)
        value_grad = value_grad + score_scale * jnp.einsum('shd,hde->she', key_block, suffix_low)
        new_state = state + jnp.einsum('thd,the->hde', query_block, grad_block)
        return (new_state, (query_grad.astype(jnp.bfloat16), key_grad.astype(jnp.bfloat16), value_grad.astype(jnp.bfloat16)))
    last_state, grads = lax.scan(backward_step, start_state, (query_blocks, key_blocks, value_blocks, grad_blocks, prefix_blocks), reverse=True)
    query_grad, key_grad, value_grad = grads
    return (query_grad.reshape(SEQ_LEN, WIDTH), key_grad.reshape(SEQ_LEN, WIDTH), value_grad.reshape(SEQ_LEN, WIDTH))
```

```python
import functools

import jax
import jax.numpy as jnp
from jax import lax
from jax.experimental import pallas as pl
from jax.experimental.pallas import tpu as pltpu
from jax.sharding import PartitionSpec as P

HEAD_DIM = 128
EPSILON = 1e-05
ROWS, COLUMNS = 8, 4
CHIPS = ROWS * COLUMNS
PEERS = CHIPS - 1
MESH = pl.DeviceIdType.MESH
F32, BF16 = jnp.float32, jnp.bfloat16


def dot(a, b, over):
    return lax.dot_general(a, b, ((over[:1], over[1:]), ((), ())), preferred_element_type=F32)


def ring_offset(k, size):
    return size // 2 + (1 - 2 * lax.rem(k, 2)) * lax.div(k + 1, 2)


def kernel(
    stacks, mine,
    q_hbm, k_hbm, v_hbm, cot_hbm, gain_ref,
    dq_hbm, dk_hbm, dv_hbm,
    tok, part, cot_own, cot_part, stage, came, scaled,
    blocks, state_out, state, gathered, scanned, prefix, low,
    weights, attended, stats, grads, late, suffix_low,
    grad_f32, grad_came, out_low,
    load_sem, store_sem, core_send, core_recv, go_send, go_recv, back_send, back_recv, stat_send, stat_recv,
):
    seq, z = lax.axis_index("seq"), lax.axis_index("head")
    core = lax.rem(seq, 2)
    other = 1 - core
    chip = lax.div(seq, 2)
    x, y = lax.rem(chip, COLUMNS), lax.div(chip, COLUMNS)
    heads = mine // HEAD_DIM
    scale = HEAD_DIM ** (-0.5)
    width = 2 * mine * stacks
    tokens = tok.shape[2]
    piece = state.shape[2]

    own_cols = pl.ds(pl.multiple_of(core * mine, mine), mine)
    part_cols = pl.ds(pl.multiple_of(other * mine, mine), mine)

    def col(j):
        return pl.ds(j * HEAD_DIM, HEAD_DIM)

    arrays = (q_hbm, k_hbm, v_hbm, cot_hbm)

    def load(a, own):
        if a == 3:
            target = cot_own if own else cot_part
        else:
            target = tok.at[a, core] if own else part.at[a]
        return pltpu.make_async_copy(
            arrays[a].at[:, own_cols if own else part_cols], target, load_sem.at[2 * a + int(own)]
        )

    for a in (1, 2):
        load(a, False).start()
    for a in (1, 2):
        load(a, True).start()
    for a in (0, 3):
        load(a, False).start()
        load(a, True).start()

    def chip_at(i):
        down = lax.rem(y + ring_offset(lax.div(i, COLUMNS), ROWS), ROWS)
        right = lax.rem(x + ring_offset(lax.rem(i, COLUMNS), COLUMNS), COLUMNS)
        return down * COLUMNS + right

    def stack_at(i):
        return {
            "seq": 2 * chip + lax.rem(core + lax.rem(i + 1, 2), 2),
            "head": lax.rem(z + lax.div(i + 1, 2), stacks),
        }

    stack_peers = 2 * stacks - 1

    def each(count, action):
        lax.fori_loop(0, count, lambda i, none: (action(i), none)[1], 0)

    barrier = pltpu.get_barrier_semaphore()

    def greet(target):
        pl.semaphore_signal(barrier, inc=1, device_id=target, device_id_type=MESH)

    each(PEERS, lambda i: greet({"seq": 2 * chip_at(i) + core, "head": z}))
    each(stack_peers, lambda i: greet(stack_at(i)))

    def to_core(src, dst, at):
        return pltpu.make_async_remote_copy(
            src_ref=src, dst_ref=dst, send_sem=core_send.at[at], recv_sem=core_recv.at[at],
            device_id={"seq": 2 * chip + other, "head": z}, device_id_type=MESH,
        )

    def go(s, i):
        target = chip_at(i)
        return pltpu.make_async_remote_copy(
            src_ref=state.at[s, target], dst_ref=gathered.at[s, chip],
            send_sem=go_send.at[s, i], recv_sem=go_recv.at[s, i],
            device_id={"seq": 2 * target + core, "head": z}, device_id_type=MESH,
        )

    def back(s, i):
        target = chip_at(i)
        return pltpu.make_async_remote_copy(
            src_ref=scanned.at[s, target], dst_ref=prefix.at[s, chip],
            send_sem=back_send.at[s, i], recv_sem=back_recv.at[s, i],
            device_id={"seq": 2 * target + core, "head": z}, device_id_type=MESH,
        )

    def scan_out(s):
        each(PEERS, lambda i: go(s, i).start())
        gathered[s, chip] = state[s, chip]

    def scan_back(s, reverse):
        each(PEERS, lambda i: go(s, i).wait_recv())
        so_far = jnp.zeros((piece, HEAD_DIM), F32)
        for p in reversed(range(CHIPS)) if reverse else range(CHIPS):
            scanned[s, p] = so_far
            so_far = so_far + gathered[s, p]
        each(PEERS, lambda i: back(s, i).start())
        prefix[s, chip] = scanned[s, chip]

    def head_of(ref, s, j):
        per_head = HEAD_DIM // piece
        return ref[s, pl.ds(j * per_head, per_head)].reshape(HEAD_DIM, HEAD_DIM)

    def put_state(s, j, value):
        per_head = HEAD_DIM // piece
        state[s, pl.ds(j * per_head, per_head)] = value.reshape(per_head, piece, HEAD_DIM)

    for a in (1, 2):
        load(a, False).wait()
    for j in range(heads):
        state_out[j] = dot(part[1, :, col(j)], part[2, :, col(j)], (0, 0))
    pl.semaphore_wait(barrier, PEERS + stack_peers)
    to_core(state_out, blocks.at[core], 0).start()
    for a in (1, 2):
        load(a, True).wait()
    for j in range(heads):
        blocks[core, j] = dot(tok[1, core, :, col(j)], tok[2, core, :, col(j)], (0, 0))
    to_core(state_out, blocks.at[other], 0).wait_recv()
    for j in range(heads):
        put_state(0, j, blocks[0, j] + blocks[1, j])
    scan_out(0)

    for n, a in enumerate((1, 2, 0)):
        if a == 0:
            load(0, False).wait()
        stage[n] = part[a].astype(F32)
        to_core(stage.at[n], came.at[n], 1 + n).start()
    load(3, False).wait()
    stage[3] = cot_part[...].astype(F32)
    to_core(stage.at[3], came.at[3], 4).start()

    causal = lax.broadcasted_iota(jnp.int32, (tokens, tokens), 0) >= lax.broadcasted_iota(
        jnp.int32, (tokens, tokens), 1
    )

    def masked(product):
        return jnp.where(causal, product * scale, 0.0).astype(BF16)

    def gain_of(j):
        return gain_ref[pl.ds(core * heads + j, 1), :]

    def within_block(b):
        for j in range(heads):
            w = masked(dot(tok[0, b, :, col(j)], tok[1, b, :, col(j)], (1, 1)))
            weights[b, :, col(j)] = w
            attended[b, :, col(j)] = dot(w, tok[2, b, :, col(j)], (1, 0))

    load(0, True).wait()
    load(3, True).wait()
    for j in range(heads):
        scaled[core, :, col(j)] = cot_own[:, col(j)].astype(F32) * gain_of(j)
    within_block(core)

    scan_back(0, False)
    for n, a in enumerate((1, 2, 0)):
        to_core(stage.at[n], came.at[n], 1 + n).wait_recv()
        tok[a, other] = came[n].astype(BF16)
    to_core(stage.at[3], came.at[3], 4).wait_recv()
    for j in range(heads):
        scaled[other, :, col(j)] = came[3, :, col(j)] * gain_of(j)
    within_block(other)

    each(PEERS, lambda i: back(0, i).wait_recv())
    squares = [jnp.zeros((tokens, HEAD_DIM), F32) for _ in range(2)]
    crosses = [jnp.zeros((tokens, HEAD_DIM), F32) for _ in range(2)]
    for j in range(heads):
        before = head_of(prefix, 0, j)
        low[0, j] = before.astype(BF16)
        low[1, j] = (before + blocks[0, j]).astype(BF16)
        for b in range(2):
            att = attended[b, :, col(j)] + scale * dot(tok[0, b, :, col(j)], low[b, j], (1, 0))
            attended[b, :, col(j)] = att
            squares[b] = squares[b] + att * att
            crosses[b] = crosses[b] + att * scaled[b, :, col(j)]
    me = 2 * z + core
    for r, sums in enumerate(squares + crosses):
        stats[me, pl.ds(r, 1), :] = jnp.sum(sums.T, axis=0, keepdims=True)

    def share(i):
        return pltpu.make_async_remote_copy(
            src_ref=stats.at[me], dst_ref=stats.at[me], send_sem=stat_send.at[i], recv_sem=stat_recv.at[i],
            device_id=stack_at(i), device_id_type=MESH,
        )

    def share_in(i):
        return pltpu.make_async_remote_copy(
            src_ref=stats.at[me], dst_ref=stats.at[me], send_sem=stat_send.at[i], recv_sem=stat_recv.at[i],
            device_id=stack_at(i), device_id_type=MESH,
        )

    each(stack_peers, lambda i: share(i).start())
    each(stack_peers, lambda i: share_in(i).wait_recv())
    total = stats[0]
    for p in range(1, 2 * stacks):
        total = total + stats[p]
    inverse_rms = lax.rsqrt(total[0:2] / width + EPSILON)
    cross_mean = total[2:4] * inverse_rms / width

    def down(row):
        return jnp.broadcast_to(row, (HEAD_DIM, tokens)).T

    inverse = [down(inverse_rms[b : b + 1]) for b in range(2)]
    cross = [down(cross_mean[b : b + 1]) for b in range(2)]
    for j in range(heads):
        sums = []
        for b in range(2):
            normed = attended[b, :, col(j)] * inverse[b]
            grad = ((scaled[b, :, col(j)] - normed * cross[b]) * inverse[b]).astype(BF16)
            grads[b, :, col(j)] = grad
            sums.append(dot(tok[0, b, :, col(j)], grad, (0, 0)))
        late[j] = sums[1]
        put_state(1, j, sums[0] + sums[1])
    scan_out(1)

    def without_suffix(b):
        for j in range(heads):
            grad = grads[b, :, col(j)]
            gw = masked(dot(grad, tok[2, b, :, col(j)], (1, 1)))
            grad_f32[0, b, :, col(j)] = dot(gw, tok[1, b, :, col(j)], (1, 0)) + scale * dot(
                grad, low[b, j], (1, 1)
            )
            grad_f32[1, b, :, col(j)] = dot(gw, tok[0, b, :, col(j)], (0, 0))
            grad_f32[2, b, :, col(j)] = dot(weights[b, :, col(j)], grad, (0, 0))

    outputs = (dq_hbm, dk_hbm, dv_hbm)

    def give(n):
        return to_core(grad_f32.at[n, other], grad_came.at[n], 5 + n)

    def store(n, own):
        return pltpu.make_async_copy(
            out_low.at[n, 0 if own else 1], outputs[n].at[:, own_cols if own else part_cols],
            store_sem.at[2 * n + int(own)],
        )

    without_suffix(other)
    give(0).start()
    without_suffix(core)
    out_low[0, 0] = grad_f32[0, core].astype(BF16)
    store(0, True).start()

    scan_back(1, True)
    give(0).wait_recv()
    out_low[0, 1] = grad_came[0].astype(BF16)
    store(0, False).start()

    each(PEERS, lambda i: back(1, i).wait_recv())
    for j in range(heads):
        after = head_of(prefix, 1, j)
        suffix_low[0, j] = (after + late[j]).astype(BF16)
        suffix_low[1, j] = after.astype(BF16)

    def with_suffix(b):
        for j in range(heads):
            suffix = suffix_low[b, j]
            grad_f32[1, b, :, col(j)] += scale * dot(tok[2, b, :, col(j)], suffix, (1, 1))
            grad_f32[2, b, :, col(j)] += scale * dot(tok[1, b, :, col(j)], suffix, (1, 0))

    with_suffix(other)
    for n in (1, 2):
        give(n).start()
    with_suffix(core)
    for n in (1, 2):
        out_low[n, 0] = grad_f32[n, core].astype(BF16)
        store(n, True).start()
    for n in (1, 2):
        give(n).wait_recv()
        out_low[n, 1] = grad_came[n].astype(BF16)
        store(n, False).start()

    to_core(state_out, blocks.at[core], 0).wait_send()
    for n in range(4):
        to_core(stage.at[n], came.at[n], 1 + n).wait_send()
    for s in range(2):
        each(PEERS, lambda i: go(s, i).wait_send())
        each(PEERS, lambda i: back(s, i).wait_send())
    each(stack_peers, lambda i: share(i).wait_send())
    for n in range(3):
        give(n).wait_send()
        store(n, True).wait()
        store(n, False).wait()


def per_device(stacks, queries, keys, values, cotangent, gain):
    tokens, local = queries.shape
    mine = local // 2
    heads = mine // HEAD_DIM
    piece = heads * HEAD_DIM // CHIPS
    anywhere = pl.BlockSpec(memory_space=pl.ANY)
    out = jax.ShapeDtypeStruct((tokens, local), BF16)
    dma = pltpu.SemaphoreType.DMA
    return pl.pallas_call(
        functools.partial(kernel, stacks, mine),
        out_shape=(out, out, out),
        in_specs=[anywhere] * 4 + [pl.BlockSpec(memory_space=pltpu.VMEM)],
        out_specs=(anywhere,) * 3,
        scratch_shapes=[
            pltpu.VMEM((3, 2, tokens, mine), BF16),
            pltpu.VMEM((3, tokens, mine), BF16),
            pltpu.VMEM((tokens, mine), BF16),
            pltpu.VMEM((tokens, mine), BF16),
            pltpu.VMEM((4, tokens, mine), F32),
            pltpu.VMEM((4, tokens, mine), F32),
            pltpu.VMEM((2, tokens, mine), F32),
            pltpu.VMEM((2, heads, HEAD_DIM, HEAD_DIM), F32),
            pltpu.VMEM((heads, HEAD_DIM, HEAD_DIM), F32),
            pltpu.VMEM((2, CHIPS, piece, HEAD_DIM), F32),
            pltpu.VMEM((2, CHIPS, piece, HEAD_DIM), F32),
            pltpu.VMEM((2, CHIPS, piece, HEAD_DIM), F32),
            pltpu.VMEM((2, CHIPS, piece, HEAD_DIM), F32),
            pltpu.VMEM((2, heads, HEAD_DIM, HEAD_DIM), BF16),
            pltpu.VMEM((2, tokens, mine), BF16),
            pltpu.VMEM((2, tokens, mine), F32),
            pltpu.VMEM((2 * stacks, 4, tokens), F32),
            pltpu.VMEM((2, tokens, mine), BF16),
            pltpu.VMEM((heads, HEAD_DIM, HEAD_DIM), F32),
            pltpu.VMEM((2, heads, HEAD_DIM, HEAD_DIM), BF16),
            pltpu.VMEM((3, 2, tokens, mine), F32),
            pltpu.VMEM((3, tokens, mine), F32),
            pltpu.VMEM((3, 2, tokens, mine), BF16),
            dma((8,)), dma((6,)),
            dma((8,)), dma((8,)),
            dma((2, PEERS)), dma((2, PEERS)), dma((2, PEERS)), dma((2, PEERS)),
            dma((2 * stacks - 1,)), dma((2 * stacks - 1,)),
        ],
        compiler_params=pltpu.CompilerParams(collective_id=0, has_side_effects=True),
        name="attention",
    )(queries, keys, values, cotangent, gain.reshape(2 * heads, HEAD_DIM))


def solution(mesh):
    spec = P("seq", "head")
    return jax.shard_map(
        functools.partial(per_device, mesh.shape["head"]),
        mesh=mesh,
        in_specs=(spec, spec, spec, spec, P("head")),
        out_specs=(spec, spec, spec),
        check_vma=False,
    )
```

```python
import functools

import jax
import jax.numpy as jnp
from jax import lax
from jax.experimental import pallas as pl
from jax.experimental.pallas import tpu as pltpu
from jax.sharding import PartitionSpec as P

HEAD_DIM = 128
EPSILON = 1e-05
ROWS, COLUMNS = 8, 4
CHIPS = ROWS * COLUMNS
PEERS = CHIPS - 1
CHUNKS = 2
MESH = pl.DeviceIdType.MESH
F32, BF16 = jnp.float32, jnp.bfloat16


def dot(a, b, over):
    return lax.dot_general(a, b, ((over[:1], over[1:]), ((), ())), preferred_element_type=F32)


def ring_offsets(size):
    return sorted(range(size), key=lambda d: -min(d, size - d))


def kernel(
    stacks, mine,
    q_hbm, k_hbm, v_hbm, cot_hbm, gain_hbm,
    result,
    gain, tok, part, cot_own, cot_part, stage, came, scaled,
    blocks, state_out, state, gathered, scanned, prefix, low,
    weights, attended, stats, grads, late,
    grad_f32, grad_came,
    load_sem, core_send, core_recv, go_send, go_recv, back_send, back_recv, stat_send, stat_recv,
):
    seq, z = lax.axis_index("seq"), lax.axis_index("head")
    core = lax.rem(seq, 2)
    other = 1 - core
    chip = lax.div(seq, 2)
    x, y = lax.rem(chip, COLUMNS), lax.div(chip, COLUMNS)
    heads = mine // HEAD_DIM
    per_chunk = heads // CHUNKS
    scale = HEAD_DIM ** (-0.5)
    width = 2 * mine * stacks
    tokens = tok.shape[2]
    piece = state.shape[3]
    per_head = HEAD_DIM // piece

    own_cols = pl.ds(pl.multiple_of(core * mine, mine), mine)
    part_cols = pl.ds(pl.multiple_of(other * mine, mine), mine)

    def col(j):
        return pl.ds(j * HEAD_DIM, HEAD_DIM)

    def heads_of(chunk):
        return range(chunk * per_chunk, (chunk + 1) * per_chunk)

    arrays = (q_hbm, k_hbm, v_hbm, cot_hbm)

    def load(a, own):
        if a == 3:
            target = cot_own if own else cot_part
        else:
            target = tok.at[a, core] if own else part.at[a]
        return pltpu.make_async_copy(
            arrays[a].at[:, own_cols if own else part_cols], target, load_sem.at[2 * a + int(own)]
        )

    load_gain = pltpu.make_async_copy(gain_hbm, gain, load_sem.at[8])
    for a in (1, 2):
        load(a, False).start()
    for a in (1, 2):
        load(a, True).start()
    for a in (0, 3):
        load(a, False).start()
        load(a, True).start()
    load_gain.start()

    down_at = [lax.rem(y + d, ROWS) * COLUMNS for d in ring_offsets(ROWS)]
    right_at = [lax.rem(x + d, COLUMNS) for d in ring_offsets(COLUMNS)]

    def other_chips():
        for k in range(ROWS):
            for m in range(COLUMNS):
                if k * COLUMNS + m < PEERS:
                    yield down_at[k] + right_at[m]

    def stack_at(i):
        return {
            "seq": 2 * chip + (core if (i + 1) % 2 == 0 else other),
            "head": lax.rem(z + (i + 1) // 2, stacks),
        }

    stack_peers = 2 * stacks - 1
    partner = {"seq": 2 * chip + other, "head": z}
    barrier = pltpu.get_barrier_semaphore()

    def greet(target):
        pl.semaphore_signal(barrier, inc=1, device_id=target, device_id_type=MESH)

    for target in other_chips():
        greet({"seq": 2 * target + core, "head": z})
    for i in range(stack_peers):
        greet(stack_at(i))

    def remote(src, dst, send, recv, device):
        return pltpu.make_async_remote_copy(
            src_ref=src, dst_ref=dst, send_sem=send, recv_sem=recv, device_id=device, device_id_type=MESH
        )

    def to_core(src, dst, at):
        return remote(src, dst, core_send.at[at], core_recv.at[at], partner)

    def exchange(src, dst, s, chunk, send, recv):
        for target in other_chips():
            remote(
                src.at[s, chunk, target], dst.at[s, chunk, chip], send.at[s, chunk], recv.at[s, chunk],
                {"seq": 2 * target + core, "head": z},
            ).start()

    def whole(ref, s, chunk, send, recv):
        span = ref.at[s, chunk, pl.ds(0, PEERS)]
        return remote(span, span, send.at[s, chunk], recv.at[s, chunk], partner)

    def scan_out(s, chunk):
        exchange(state, gathered, s, chunk, go_send, go_recv)
        gathered[s, chunk, chip] = state[s, chunk, chip]

    def scan_back(s, chunk, reverse):
        with jax.named_scope(f"go_wait{s}{chunk}"):
            whole(gathered, s, chunk, go_send, go_recv).wait_recv()
        with jax.named_scope(f"scan{s}{chunk}"):
            so_far = jnp.zeros((piece, HEAD_DIM), F32)
            for p in reversed(range(CHIPS)) if reverse else range(CHIPS):
                scanned[s, chunk, p] = so_far
                so_far = so_far + gathered[s, chunk, p]
        with jax.named_scope(f"back_start{s}{chunk}"):
            exchange(scanned, prefix, s, chunk, back_send, back_recv)
            prefix[s, chunk, chip] = scanned[s, chunk, chip]

    def scan_in(s, chunk):
        with jax.named_scope(f"back_wait{s}{chunk}"):
            whole(prefix, s, chunk, back_send, back_recv).wait_recv()

    def head_of(s, j):
        at = pl.ds(j % per_chunk * per_head, per_head)
        return prefix[s, j // per_chunk, at].reshape(HEAD_DIM, HEAD_DIM)

    def put_state(s, j, value):
        at = pl.ds(j % per_chunk * per_head, per_head)
        state[s, j // per_chunk, at] = value.reshape(per_head, piece, HEAD_DIM)

    def give_states(chunk):
        at = pl.ds(chunk * per_chunk, per_chunk)
        return to_core(state_out.at[at], blocks.at[core, at], chunk)

    def take_states(chunk):
        at = pl.ds(chunk * per_chunk, per_chunk)
        return to_core(state_out.at[at], blocks.at[other, at], chunk)

    def part_states(chunk):
        for j in heads_of(chunk):
            state_out[j] = dot(part[1, :, col(j)], part[2, :, col(j)], (0, 0))

    with jax.named_scope("load_wait"):
        for a in (1, 2):
            load(a, False).wait()
    with jax.named_scope("states_a"):
        part_states(0)
    with jax.named_scope("barrier"):
        pl.semaphore_wait(barrier, PEERS + stack_peers)
    give_states(0).start()
    for chunk in range(1, CHUNKS):
        part_states(chunk)
        give_states(chunk).start()
    with jax.named_scope("states_b"):
        for a in (1, 2):
            load(a, True).wait()
        for j in range(heads):
            blocks[core, j] = dot(tok[1, core, :, col(j)], tok[2, core, :, col(j)], (0, 0))
    for chunk in range(CHUNKS):
        with jax.named_scope(f"core_wait{chunk}"):
            take_states(chunk).wait_recv()
        with jax.named_scope(f"go0{chunk}"):
            for j in heads_of(chunk):
                put_state(0, j, blocks[0, j] + blocks[1, j])
            scan_out(0, chunk)

    def give_tokens(n):
        return to_core(stage.at[n], came.at[n], CHUNKS + n)

    with jax.named_scope("stage"):
        for n, a in enumerate((1, 2, 0)):
            if a == 0:
                load(0, False).wait()
            stage[n] = part[a].astype(F32)
            give_tokens(n).start()
        load(3, False).wait()
        stage[3] = cot_part[...].astype(F32)
        give_tokens(3).start()

    causal = lax.broadcasted_iota(jnp.int32, (tokens, tokens), 0) >= lax.broadcasted_iota(
        jnp.int32, (tokens, tokens), 1
    )

    def masked(product):
        return jnp.where(causal, product * scale, 0.0).astype(BF16)

    def gain_of(j):
        return gain[pl.ds(core * heads + j, 1), :]

    def within_block(b):
        for j in range(heads):
            w = masked(dot(tok[0, b, :, col(j)], tok[1, b, :, col(j)], (1, 1)))
            weights[b, :, col(j)] = w
            attended[b, :, col(j)] = dot(w, tok[2, b, :, col(j)], (1, 0))

    with jax.named_scope("within_own"):
        load(0, True).wait()
        load(3, True).wait()
        load_gain.wait()
        for j in range(heads):
            scaled[core, :, col(j)] = cot_own[:, col(j)].astype(F32) * gain_of(j)
        within_block(core)
    with jax.named_scope("within_other"):
        for n, a in enumerate((1, 2, 0)):
            give_tokens(n).wait_recv()
            tok[a, other] = came[n].astype(BF16)
        give_tokens(3).wait_recv()
        for j in range(heads):
            scaled[other, :, col(j)] = came[3, :, col(j)] * gain_of(j)
        within_block(other)

    for chunk in range(CHUNKS):
        scan_back(0, chunk, False)

    squares = [jnp.zeros((tokens, HEAD_DIM), F32) for _ in range(2)]
    crosses = [jnp.zeros((tokens, HEAD_DIM), F32) for _ in range(2)]
    for chunk in range(CHUNKS):
        scan_in(0, chunk)
        with jax.named_scope(f"attended{chunk}"):
            for j in heads_of(chunk):
                before = head_of(0, j)
                low[0, j] = before.astype(BF16)
                low[1, j] = (before + blocks[0, j]).astype(BF16)
                for b in range(2):
                    att = attended[b, :, col(j)] + scale * dot(tok[0, b, :, col(j)], low[b, j], (1, 0))
                    attended[b, :, col(j)] = att
                    squares[b] = squares[b] + att * att
                    crosses[b] = crosses[b] + att * scaled[b, :, col(j)]
    me = 2 * z + core
    with jax.named_scope("statsum"):
        for r, sums in enumerate(squares + crosses):
            stats[me, pl.ds(r, 1), :] = jnp.sum(sums.T, axis=0, keepdims=True)
        for i in range(stack_peers):
            remote(stats.at[me], stats.at[me], stat_send, stat_recv, stack_at(i)).start()
    rest = stats.at[pl.ds(0, stack_peers)]
    all_stats = remote(rest, rest, stat_send, stat_recv, partner)
    with jax.named_scope("stat_wait"):
        all_stats.wait_recv()
    with jax.named_scope("stat_use"):
        total = stats[0]
        for p in range(1, 2 * stacks):
            total = total + stats[p]
        inverse_rms = lax.rsqrt(total[0:2] / width + EPSILON)
        cross_mean = total[2:4] * inverse_rms / width

        def down(row):
            return jnp.broadcast_to(row, (HEAD_DIM, tokens)).T

        inverse = [down(inverse_rms[b : b + 1]) for b in range(2)]
        cross = [down(cross_mean[b : b + 1]) for b in range(2)]
    for chunk in range(CHUNKS):
        with jax.named_scope(f"grads{chunk}"):
            for j in heads_of(chunk):
                sums = []
                for b in range(2):
                    normed = attended[b, :, col(j)] * inverse[b]
                    grad = ((scaled[b, :, col(j)] - normed * cross[b]) * inverse[b]).astype(BF16)
                    grads[b, :, col(j)] = grad
                    sums.append(dot(tok[0, b, :, col(j)], grad, (0, 0)))
                late[j] = sums[1]
                put_state(1, j, sums[0] + sums[1])
        with jax.named_scope(f"go1{chunk}"):
            scan_out(1, chunk)

    def without_suffix(b):
        for j in range(heads):
            grad = grads[b, :, col(j)]
            gw = masked(dot(grad, tok[2, b, :, col(j)], (1, 1)))
            grad_f32[0, b, :, col(j)] = dot(gw, tok[1, b, :, col(j)], (1, 0)) + scale * dot(
                grad, low[b, j], (1, 1)
            )
            grad_f32[1, b, :, col(j)] = dot(gw, tok[0, b, :, col(j)], (0, 0))
            grad_f32[2, b, :, col(j)] = dot(weights[b, :, col(j)], grad, (0, 0))

    base = CHUNKS + 4
    give_query = to_core(grad_f32.at[0, other], grad_came.at[0], base)

    def give(n, chunk):
        at = pl.ds(chunk * per_chunk * HEAD_DIM, per_chunk * HEAD_DIM)
        return to_core(grad_f32.at[n, other, :, at], grad_came.at[n, :, at], base + 1 + 2 * chunk + n - 1)

    with jax.named_scope("without_suffix"):
        without_suffix(other)
        give_query.start()
        without_suffix(core)
        result[0, :, own_cols] = grad_f32[0, core].astype(BF16)
    with jax.named_scope("dq_out"):
        give_query.wait_recv()
        result[0, :, part_cols] = grad_came[0].astype(BF16)

    for chunk in range(CHUNKS):
        scan_back(1, chunk, True)

    def with_suffix(b, j, suffix):
        grad_f32[1, b, :, col(j)] += scale * dot(tok[2, b, :, col(j)], suffix, (1, 1))
        grad_f32[2, b, :, col(j)] += scale * dot(tok[1, b, :, col(j)], suffix, (1, 0))

    for chunk in range(CHUNKS):
        scan_in(1, chunk)
        with jax.named_scope(f"with_suffix{chunk}"):
            for j in heads_of(chunk):
                after = head_of(1, j)
                with_suffix(0, j, (after + late[j]).astype(BF16))
                with_suffix(1, j, after.astype(BF16))
            for n in (1, 2):
                give(n, chunk).start()
    with jax.named_scope("own_out"):
        for n in (1, 2):
            result[n, :, own_cols] = grad_f32[n, core].astype(BF16)

    with jax.named_scope("send_waits"):
        for chunk in range(CHUNKS):
            give_states(chunk).wait_send()
        for n in range(4):
            give_tokens(n).wait_send()
        for s in range(2):
            for chunk in range(CHUNKS):
                whole(state, s, chunk, go_send, go_recv).wait_send()
                whole(scanned, s, chunk, back_send, back_recv).wait_send()
        all_stats.wait_send()
        give_query.wait_send()
    with jax.named_scope("final_core"):
        for chunk in range(CHUNKS):
            for n in (1, 2):
                give(n, chunk).wait_recv()
        for n in (1, 2):
            result[n, :, part_cols] = grad_came[n].astype(BF16)
        for chunk in range(CHUNKS):
            for n in (1, 2):
                give(n, chunk).wait_send()


def write_out(result, dq_hbm, dk_hbm, dv_hbm, sems):
    copies = [
        pltpu.make_async_copy(result.at[n], out, sems.at[n]) for n, out in enumerate((dq_hbm, dk_hbm, dv_hbm))
    ]
    for copy in copies:
        copy.start()
    for copy in copies:
        copy.wait()


def per_device(stacks, queries, keys, values, cotangent, gain):
    tokens, local = queries.shape
    mine = local // 2
    heads = mine // HEAD_DIM
    piece = heads * HEAD_DIM // CHIPS // CHUNKS
    anywhere = pl.BlockSpec(memory_space=pl.ANY)
    vmem = pl.BlockSpec(memory_space=pltpu.VMEM)
    dma = pltpu.SemaphoreType.DMA
    arrays = (queries, keys, values, cotangent, gain.reshape(2 * heads, HEAD_DIM))
    result = pl.pallas_call(
        functools.partial(kernel, stacks, mine),
        out_shape=jax.ShapeDtypeStruct((3, tokens, local), BF16),
        in_specs=[pl.BlockSpec(memory_space=pltpu.HBM)] * 5,
        out_specs=vmem,
        scratch_shapes=[
            pltpu.VMEM((2 * heads, HEAD_DIM), F32),
            pltpu.VMEM((3, 2, tokens, mine), BF16),
            pltpu.VMEM((3, tokens, mine), BF16),
            pltpu.VMEM((tokens, mine), BF16),
            pltpu.VMEM((tokens, mine), BF16),
            pltpu.VMEM((4, tokens, mine), F32),
            pltpu.VMEM((4, tokens, mine), F32),
            pltpu.VMEM((2, tokens, mine), F32),
            pltpu.VMEM((2, heads, HEAD_DIM, HEAD_DIM), F32),
            pltpu.VMEM((heads, HEAD_DIM, HEAD_DIM), F32),
            pltpu.VMEM((2, CHUNKS, CHIPS, piece, HEAD_DIM), F32),
            pltpu.VMEM((2, CHUNKS, CHIPS, piece, HEAD_DIM), F32),
            pltpu.VMEM((2, CHUNKS, CHIPS, piece, HEAD_DIM), F32),
            pltpu.VMEM((2, CHUNKS, CHIPS, piece, HEAD_DIM), F32),
            pltpu.VMEM((2, heads, HEAD_DIM, HEAD_DIM), BF16),
            pltpu.VMEM((2, tokens, mine), BF16),
            pltpu.VMEM((2, tokens, mine), F32),
            pltpu.VMEM((2 * stacks, 4, tokens), F32),
            pltpu.VMEM((2, tokens, mine), BF16),
            pltpu.VMEM((heads, HEAD_DIM, HEAD_DIM), F32),
            pltpu.VMEM((3, 2, tokens, mine), F32),
            pltpu.VMEM((3, tokens, mine), F32),
            dma((9,)),
            dma((5 + 3 * CHUNKS,)), dma((5 + 3 * CHUNKS,)),
            dma((2, CHUNKS)), dma((2, CHUNKS)), dma((2, CHUNKS)), dma((2, CHUNKS)),
            dma, dma,
        ],
        compiler_params=pltpu.CompilerParams(
            collective_id=0, has_side_effects=True, vmem_limit_bytes=24 * 1024 * 1024
        ),
        name="attention",
    )(*(pltpu.with_memory_space_constraint(a, pltpu.HBM) for a in arrays))
    out = jax.ShapeDtypeStruct((tokens, local), BF16)
    return pl.pallas_call(
        write_out,
        out_shape=(out, out, out),
        in_specs=[vmem],
        out_specs=(anywhere,) * 3,
        scratch_shapes=[dma((3,))],
        compiler_params=pltpu.CompilerParams(vmem_limit_bytes=4 * 1024 * 1024),
        name="write_out",
    )(result)


def solution(mesh):
    spec = P("seq", "head")
    return jax.shard_map(
        functools.partial(per_device, mesh.shape["head"]),
        mesh=mesh,
        in_specs=(spec, spec, spec, spec, P("head")),
        out_specs=(spec, spec, spec),
        check_vma=False,
    )
```

```python
import functools

import jax
import jax.numpy as jnp
from jax import lax
from jax.experimental import pallas as pl
from jax.experimental.pallas import tpu as pltpu
from jax.sharding import PartitionSpec as P

HEAD_DIM = 128
EPSILON = 1e-05
ROWS, COLUMNS = 8, 4
CHIPS = ROWS * COLUMNS
CHUNKS = 2
MESH = pl.DeviceIdType.MESH
F32, BF16 = jnp.float32, jnp.bfloat16


def dot(a, b, over):
    return lax.dot_general(a, b, ((over[:1], over[1:]), ((), ())), preferred_element_type=F32)


def ring_offsets(size):
    return sorted(range(size), key=lambda d: -min(d, size - d))


def kernel(
    stacks, mine,
    q_hbm, k_hbm, v_hbm, cot_hbm, gain_hbm,
    result,
    gain, tok, part, cot_own, cot_part, stage, came, scaled,
    blocks, state_out, state, gathered, scanned, prefix, low,
    weights, attended, stats, grads, late,
    grad_f32, grad_came,
    load_sem, core_send, core_recv, go_send, go_recv, back_send, back_recv, stat_send, stat_recv,
    met, stack_ready,
):
    seq, z = lax.axis_index("seq"), lax.axis_index("head")
    core = lax.rem(seq, 2)
    other = 1 - core
    chip = lax.div(seq, 2)
    x, y = lax.rem(chip, COLUMNS), lax.div(chip, COLUMNS)
    heads = mine // HEAD_DIM
    per_chunk = heads // CHUNKS
    scale = HEAD_DIM ** (-0.5)
    width = 2 * mine * stacks
    tokens = tok.shape[2]
    piece = state.shape[3]
    per_head = HEAD_DIM // piece

    own_cols = pl.ds(pl.multiple_of(core * mine, mine), mine)
    part_cols = pl.ds(pl.multiple_of(other * mine, mine), mine)

    def col(j):
        return pl.ds(j * HEAD_DIM, HEAD_DIM)

    def heads_of(chunk):
        return range(chunk * per_chunk, (chunk + 1) * per_chunk)

    arrays = (q_hbm, k_hbm, v_hbm, cot_hbm)

    def load(a, own):
        if a == 3:
            target = cot_own if own else cot_part
        else:
            target = tok.at[a, core] if own else part.at[a]
        return pltpu.make_async_copy(
            arrays[a].at[:, own_cols if own else part_cols], target, load_sem.at[2 * a + int(own)]
        )

    load_gain = pltpu.make_async_copy(gain_hbm, gain, load_sem.at[8])
    with jax.named_scope("load_first"):
        for a in (1, 2):
            load(a, False).start()

    down_at = [lax.rem(y + d, ROWS) * COLUMNS for d in ring_offsets(ROWS)]
    right_at = [lax.rem(x + d, COLUMNS) for d in ring_offsets(COLUMNS)]
    offsets = [(d, r) for d in range(ROWS) for r in range(COLUMNS)]
    all_chips = [down_at[d] + right_at[r] for d, r in offsets]
    odd = [(ring_offsets(ROWS)[d] + ring_offsets(COLUMNS)[r]) % 2 for d, r in offsets]
    colour = lax.rem(x + y, 2)

    def place(target, its_colour):
        return its_colour * (CHIPS // 2) + lax.div(target, 2)

    my_place = place(chip, colour)

    def owners(wanted):
        for target, is_odd in zip(all_chips, odd):
            if is_odd == wanted:
                yield target

    partner = {"seq": 2 * chip + other, "head": z}
    barrier = pltpu.get_barrier_semaphore()

    def tell(sem, target):
        pl.semaphore_signal(sem, inc=1, device_id=target, device_id_type=MESH)

    with jax.named_scope("greet"):
        for target in all_chips[:-1]:
            tell(barrier, {"seq": 2 * target + 1, "head": z})

        @pl.when(core == 1)
        def _():
            tell(barrier, partner)

        for plane in range(1, stacks):

            @pl.when(plane > z)
            def _():
                tell(barrier, {"seq": 2 * chip + 1, "head": plane})

    def meet_partner():
        @pl.when(core == 0)
        def _():
            pl.semaphore_wait(barrier, 1)
            tell(met, partner)

        @pl.when(core == 1)
        def _():
            pl.semaphore_wait(met, 1)

    def meet_plane():
        @pl.when(core == 1)
        def _():
            pl.semaphore_wait(barrier, 2 * (CHIPS - 1) + 2 * z)
            tell(met, partner)
            for plane in range(stacks - 1):

                @pl.when(plane < z)
                def _():
                    tell(stack_ready, {"seq": 2 * chip, "head": plane})
                    tell(stack_ready, {"seq": 2 * chip + 1, "head": plane})

        @pl.when(core == 0)
        def _():
            pl.semaphore_wait(met, 1)

    with jax.named_scope("load_rest"):
        for a in (1, 2):
            load(a, True).start()
        for a in (0, 3):
            load(a, False).start()
            load(a, True).start()
        load_gain.start()

    def remote(src, dst, send, recv, device):
        return pltpu.make_async_remote_copy(
            src_ref=src, dst_ref=dst, send_sem=send, recv_sem=recv, device_id=device, device_id_type=MESH
        )

    def to_core(src, dst, at):
        return remote(src, dst, core_send.at[at], core_recv.at[at], partner)

    def go(s, chunk):
        for first in range(2):

            @pl.when(colour == first)
            def _():
                for head in range(2):
                    for target in owners((head + first) % 2):
                        remote(
                            state.at[s, chunk, place(target, head)], gathered.at[s, chunk, chip],
                            go_send.at[s, chunk], go_recv.at[s, chunk], {"seq": 2 * target + other, "head": z},
                        ).start()

    def back(s, chunk):
        for target in all_chips:
            remote(
                scanned.at[s, chunk, target], prefix.at[s, chunk, my_place],
                back_send.at[s, chunk], back_recv.at[s, chunk, colour], {"seq": 2 * target + other, "head": z},
            ).start()

    def whole(ref, s, chunk, send, recv):
        span = ref.at[s, chunk]
        return remote(span, span, send.at[s, chunk], recv, partner)

    def scan_back(s, chunk, reverse):
        with jax.named_scope(f"go_wait{s}{chunk}"):
            whole(gathered, s, chunk, go_send, go_recv.at[s, chunk]).wait_recv()
        with jax.named_scope(f"scan{s}{chunk}"):
            so_far = jnp.zeros((piece, HEAD_DIM), F32)
            for p in reversed(range(CHIPS)) if reverse else range(CHIPS):
                scanned[s, chunk, p] = so_far
                so_far = so_far + gathered[s, chunk, p]
        with jax.named_scope(f"back_start{s}{chunk}"):
            back(s, chunk)

    def scan_in(s, j):
        half = prefix.at[s, j // 2, pl.ds(j % 2 * (CHIPS // 2), CHIPS // 2)]
        with jax.named_scope(f"back_wait{s}{j}"):
            remote(half, half, back_send.at[s, j // 2], back_recv.at[s, j // 2, j % 2], partner).wait_recv()

    def head_of(s, j):
        at = pl.ds(j % per_chunk * per_head, per_head)
        return prefix[s, j // per_chunk, at].reshape(HEAD_DIM, HEAD_DIM)

    def put_state(s, j, value):
        at = pl.ds(j % per_chunk * per_head, per_head)
        state[s, j // per_chunk, at] = value.reshape(per_head, piece, HEAD_DIM)

    def give_states(chunk):
        at = pl.ds(chunk * per_chunk, per_chunk)
        return to_core(state_out.at[at], blocks.at[core, at], chunk)

    def take_states(chunk):
        at = pl.ds(chunk * per_chunk, per_chunk)
        return to_core(state_out.at[at], blocks.at[other, at], chunk)

    def part_states(chunk):
        for j in heads_of(chunk):
            state_out[j] = dot(part[1, :, col(j)], part[2, :, col(j)], (0, 0))

    with jax.named_scope("load_wait"):
        for a in (1, 2):
            load(a, False).wait()
    with jax.named_scope("states_a"):
        part_states(0)
    with jax.named_scope("meet_partner"):
        meet_partner()
    give_states(0).start()
    for chunk in range(1, CHUNKS):
        part_states(chunk)
        give_states(chunk).start()
    with jax.named_scope("states_b"):
        for a in (1, 2):
            load(a, True).wait()
        for j in range(heads):
            blocks[core, j] = dot(tok[1, core, :, col(j)], tok[2, core, :, col(j)], (0, 0))
    with jax.named_scope("core_wait"):
        for chunk in range(CHUNKS):
            take_states(chunk).wait_recv()
            for j in heads_of(chunk):
                put_state(0, j, blocks[0, j] + blocks[1, j])
    with jax.named_scope("barrier"):
        meet_plane()
    for chunk in range(CHUNKS):
        with jax.named_scope(f"go0{chunk}"):
            go(0, chunk)

    def give_tokens(n):
        return to_core(stage.at[n], came.at[n], CHUNKS + n)

    with jax.named_scope("stage"):
        for n, a in enumerate((1, 2, 0)):
            if a == 0:
                load(0, False).wait()
            stage[n] = part[a].astype(F32)
            give_tokens(n).start()
        load(3, False).wait()
        stage[3] = cot_part[...].astype(F32)
        give_tokens(3).start()

    causal = lax.broadcasted_iota(jnp.int32, (tokens, tokens), 0) >= lax.broadcasted_iota(
        jnp.int32, (tokens, tokens), 1
    )

    def masked(product):
        return jnp.where(causal, product * scale, 0.0).astype(BF16)

    def gain_of(j):
        return gain[pl.ds(core * heads + j, 1), :]

    def within_block(b):
        for j in range(heads):
            w = masked(dot(tok[0, b, :, col(j)], tok[1, b, :, col(j)], (1, 1)))
            weights[b, :, col(j)] = w
            attended[b, :, col(j)] = dot(w, tok[2, b, :, col(j)], (1, 0))

    with jax.named_scope("within_own"):
        load(0, True).wait()
        load(3, True).wait()
        load_gain.wait()
        for j in range(heads):
            scaled[core, :, col(j)] = cot_own[:, col(j)].astype(F32) * gain_of(j)
        within_block(core)
    with jax.named_scope("within_other"):
        for n, a in enumerate((1, 2, 0)):
            give_tokens(n).wait_recv()
            tok[a, other] = came[n].astype(BF16)
        give_tokens(3).wait_recv()
        for j in range(heads):
            scaled[other, :, col(j)] = came[3, :, col(j)] * gain_of(j)
        within_block(other)

    for chunk in range(CHUNKS):
        scan_back(0, chunk, False)

    squares = [jnp.zeros((tokens, HEAD_DIM), F32) for _ in range(2)]
    crosses = [jnp.zeros((tokens, HEAD_DIM), F32) for _ in range(2)]
    for head in range(heads):
        scan_in(0, head)
        with jax.named_scope(f"attended{head}"):
            for j in (head,):
                before = head_of(0, j)
                low[0, j] = before.astype(BF16)
                low[1, j] = (before + blocks[0, j]).astype(BF16)
                for b in range(2):
                    att = attended[b, :, col(j)] + scale * dot(tok[0, b, :, col(j)], low[b, j], (1, 0))
                    attended[b, :, col(j)] = att
                    squares[b] = squares[b] + att * att
                    crosses[b] = crosses[b] + att * scaled[b, :, col(j)]
    me = 2 * z + core
    with jax.named_scope("statsum"):
        for r, sums in enumerate(squares + crosses):
            stats[me, pl.ds(r, 1), :] = jnp.sum(sums.T, axis=0, keepdims=True)
        @pl.when(z < stacks - 1)
        def _():
            pl.semaphore_wait(stack_ready, stacks - 1 - z)

        for up in range(1, stacks):
            for there in (core, other):
                device = {"seq": 2 * chip + there, "head": lax.rem(z + up, stacks)}
                remote(stats.at[me], stats.at[me], stat_send, stat_recv, device).start()
        remote(stats.at[me], stats.at[me], stat_send, stat_recv, partner).start()
    rest = stats.at[pl.ds(0, 2 * stacks - 1)]
    all_stats = remote(rest, rest, stat_send, stat_recv, partner)
    with jax.named_scope("stat_wait"):
        all_stats.wait_recv()
    with jax.named_scope("stat_use"):
        total = stats[0]
        for p in range(1, 2 * stacks):
            total = total + stats[p]
        inverse_rms = lax.rsqrt(total[0:2] / width + EPSILON)
        cross_mean = total[2:4] * inverse_rms / width

        def down(row):
            return jnp.broadcast_to(row, (HEAD_DIM, tokens)).T

        inverse = [down(inverse_rms[b : b + 1]) for b in range(2)]
        cross = [down(cross_mean[b : b + 1]) for b in range(2)]
    for chunk in range(CHUNKS):
        with jax.named_scope(f"grads{chunk}"):
            for j in heads_of(chunk):
                sums = []
                for b in range(2):
                    normed = attended[b, :, col(j)] * inverse[b]
                    grad = ((scaled[b, :, col(j)] - normed * cross[b]) * inverse[b]).astype(BF16)
                    grads[b, :, col(j)] = grad
                    sums.append(dot(tok[0, b, :, col(j)], grad, (0, 0)))
                late[j] = sums[1]
                put_state(1, j, sums[0] + sums[1])
        with jax.named_scope(f"go1{chunk}"):
            go(1, chunk)

    def without_suffix(b):
        for j in range(heads):
            grad = grads[b, :, col(j)]
            gw = masked(dot(grad, tok[2, b, :, col(j)], (1, 1)))
            grad_f32[0, b, :, col(j)] = dot(gw, tok[1, b, :, col(j)], (1, 0)) + scale * dot(
                grad, low[b, j], (1, 1)
            )
            grad_f32[1, b, :, col(j)] = dot(gw, tok[0, b, :, col(j)], (0, 0))
            grad_f32[2, b, :, col(j)] = dot(weights[b, :, col(j)], grad, (0, 0))

    base = CHUNKS + 4
    give_query = to_core(grad_f32.at[0, other], grad_came.at[0], base)

    def give(n, j):
        return to_core(grad_f32.at[n, other, :, col(j)], grad_came.at[n, :, col(j)], base + 2 * j + n)

    with jax.named_scope("without_suffix"):
        without_suffix(other)
        give_query.start()
        without_suffix(core)
        result[0, :, own_cols] = grad_f32[0, core].astype(BF16)
    with jax.named_scope("dq_out"):
        give_query.wait_recv()
        result[0, :, part_cols] = grad_came[0].astype(BF16)

    for chunk in range(CHUNKS):
        scan_back(1, chunk, True)

    def with_suffix(b, j, suffix):
        grad_f32[1, b, :, col(j)] += scale * dot(tok[2, b, :, col(j)], suffix, (1, 1))
        grad_f32[2, b, :, col(j)] += scale * dot(tok[1, b, :, col(j)], suffix, (1, 0))

    for j in range(heads):
        scan_in(1, j)
        with jax.named_scope(f"with_suffix{j}"):
            after = head_of(1, j)
            with_suffix(0, j, (after + late[j]).astype(BF16))
            with_suffix(1, j, after.astype(BF16))
            for n in (1, 2):
                give(n, j).start()
    with jax.named_scope("own_out"):
        for n in (1, 2):
            result[n, :, own_cols] = grad_f32[n, core].astype(BF16)

    with jax.named_scope("send_waits"):
        for chunk in range(CHUNKS):
            give_states(chunk).wait_send()
        for n in range(4):
            give_tokens(n).wait_send()
        for s in range(2):
            for chunk in range(CHUNKS):
                whole(state, s, chunk, go_send, go_recv.at[s, chunk]).wait_send()
                whole(scanned, s, chunk, back_send, go_recv.at[s, chunk]).wait_send()
        all_stats.wait_send()
        give_query.wait_send()
    with jax.named_scope("final_core"):
        for j in range(heads):
            for n in (1, 2):
                give(n, j).wait_recv()
        for n in (1, 2):
            result[n, :, part_cols] = grad_came[n].astype(BF16)
        for j in range(heads):
            for n in (1, 2):
                give(n, j).wait_send()


def write_out(result, dq_hbm, dk_hbm, dv_hbm, sems):
    copies = [
        pltpu.make_async_copy(result.at[n], out, sems.at[n]) for n, out in enumerate((dq_hbm, dk_hbm, dv_hbm))
    ]
    for copy in copies:
        copy.start()
    for copy in copies:
        copy.wait()


def per_device(stacks, queries, keys, values, cotangent, gain):
    tokens, local = queries.shape
    mine = local // 2
    heads = mine // HEAD_DIM
    piece = heads * HEAD_DIM // CHIPS // CHUNKS
    anywhere = pl.BlockSpec(memory_space=pl.ANY)
    vmem = pl.BlockSpec(memory_space=pltpu.VMEM)
    dma = pltpu.SemaphoreType.DMA
    arrays = (queries, keys, values, cotangent, gain.reshape(2 * heads, HEAD_DIM))
    result = pl.pallas_call(
        functools.partial(kernel, stacks, mine),
        out_shape=jax.ShapeDtypeStruct((3, tokens, local), BF16),
        in_specs=[pl.BlockSpec(memory_space=pltpu.HBM)] * 5,
        out_specs=vmem,
        scratch_shapes=[
            pltpu.VMEM((2 * heads, HEAD_DIM), F32),
            pltpu.VMEM((3, 2, tokens, mine), BF16),
            pltpu.VMEM((3, tokens, mine), BF16),
            pltpu.VMEM((tokens, mine), BF16),
            pltpu.VMEM((tokens, mine), BF16),
            pltpu.VMEM((4, tokens, mine), F32),
            pltpu.VMEM((4, tokens, mine), F32),
            pltpu.VMEM((2, tokens, mine), F32),
            pltpu.VMEM((2, heads, HEAD_DIM, HEAD_DIM), F32),
            pltpu.VMEM((heads, HEAD_DIM, HEAD_DIM), F32),
            pltpu.VMEM((2, CHUNKS, CHIPS, piece, HEAD_DIM), F32),
            pltpu.VMEM((2, CHUNKS, CHIPS, piece, HEAD_DIM), F32),
            pltpu.VMEM((2, CHUNKS, CHIPS, piece, HEAD_DIM), F32),
            pltpu.VMEM((2, CHUNKS, CHIPS, piece, HEAD_DIM), F32),
            pltpu.VMEM((2, heads, HEAD_DIM, HEAD_DIM), BF16),
            pltpu.VMEM((2, tokens, mine), BF16),
            pltpu.VMEM((2, tokens, mine), F32),
            pltpu.VMEM((2 * stacks, 4, tokens), F32),
            pltpu.VMEM((2, tokens, mine), BF16),
            pltpu.VMEM((heads, HEAD_DIM, HEAD_DIM), F32),
            pltpu.VMEM((3, 2, tokens, mine), F32),
            pltpu.VMEM((3, tokens, mine), F32),
            dma((9,)),
            dma((5 + CHUNKS + 2 * heads,)), dma((5 + CHUNKS + 2 * heads,)),
            dma((2, CHUNKS)), dma((2, CHUNKS)), dma((2, CHUNKS)), dma((2, CHUNKS, 2)),
            dma, dma,
            pltpu.SemaphoreType.REGULAR, pltpu.SemaphoreType.REGULAR,
        ],
        compiler_params=pltpu.CompilerParams(
            collective_id=0, has_side_effects=True, vmem_limit_bytes=24 * 1024 * 1024
        ),
        name="attention",
    )(*(pltpu.with_memory_space_constraint(a, pltpu.HBM) for a in arrays))
    out = jax.ShapeDtypeStruct((tokens, local), BF16)
    return pl.pallas_call(
        write_out,
        out_shape=(out, out, out),
        in_specs=[vmem],
        out_specs=(anywhere,) * 3,
        scratch_shapes=[dma((3,))],
        compiler_params=pltpu.CompilerParams(vmem_limit_bytes=4 * 1024 * 1024),
        name="write_out",
    )(result)


def solution(mesh):
    spec = P("seq", "head")
    return jax.shard_map(
        functools.partial(per_device, mesh.shape["head"]),
        mesh=mesh,
        in_specs=(spec, spec, spec, spec, P("head")),
        out_specs=(spec, spec, spec),
        check_vma=False,
    )
```

```python
import functools

import jax
import jax.numpy as jnp
from jax import lax
from jax.experimental import pallas as pl
from jax.experimental.pallas import tpu as pltpu
from jax.sharding import PartitionSpec as P

HEAD_DIM = 128
EPSILON = 1e-05
ROWS, COLUMNS = 8, 4
CHIPS = ROWS * COLUMNS
CHUNKS = 2
MESH = pl.DeviceIdType.MESH
F32, BF16 = jnp.float32, jnp.bfloat16


def dot(a, b, over):
    return lax.dot_general(a, b, ((over[:1], over[1:]), ((), ())), preferred_element_type=F32)


def ring_offsets(size):
    return sorted(range(size), key=lambda d: -min(d, size - d))


def kernel(
    stacks, mine,
    q_hbm, k_hbm, v_hbm, cot_hbm, gain_hbm,
    result,
    gain, tok, part, cot_own, cot_part, stage, came, scaled,
    blocks, state_out, state, gathered, scanned, prefix, low,
    weights, attended, stats, grads, late,
    grad_f32, grad_came,
    load_sem, core_send, core_recv, go_send, go_recv, back_send, back_recv, stat_send, stat_recv,
    met, stack_ready,
):
    seq, z = lax.axis_index("seq"), lax.axis_index("head")
    core = lax.rem(seq, 2)
    other = 1 - core
    chip = lax.div(seq, 2)
    x, y = lax.rem(chip, COLUMNS), lax.div(chip, COLUMNS)
    heads = mine // HEAD_DIM
    per_chunk = heads // CHUNKS
    scale = HEAD_DIM ** (-0.5)
    width = 2 * mine * stacks
    tokens = tok.shape[2]
    piece = state.shape[3]
    per_head = HEAD_DIM // piece

    own_cols = pl.ds(pl.multiple_of(core * mine, mine), mine)
    part_cols = pl.ds(pl.multiple_of(other * mine, mine), mine)

    def col(j):
        return pl.ds(j * HEAD_DIM, HEAD_DIM)

    def heads_of(chunk):
        return range(chunk * per_chunk, (chunk + 1) * per_chunk)

    arrays = (q_hbm, k_hbm, v_hbm, cot_hbm)

    def load(a, own):
        if a == 3:
            target = cot_own if own else cot_part
        else:
            target = tok.at[a, core] if own else part.at[a]
        return pltpu.make_async_copy(
            arrays[a].at[:, own_cols if own else part_cols], target, load_sem.at[2 * a + int(own)]
        )

    load_gain = pltpu.make_async_copy(gain_hbm, gain, load_sem.at[8])
    with jax.named_scope("load_first"):
        for a in (1, 2):
            load(a, False).start()

    down_at = [lax.rem(y + d, ROWS) * COLUMNS for d in ring_offsets(ROWS)]
    right_at = [lax.rem(x + d, COLUMNS) for d in ring_offsets(COLUMNS)]
    offsets = [(d, r) for d in range(ROWS) for r in range(COLUMNS)]
    all_chips = [down_at[d] + right_at[r] for d, r in offsets]
    odd = [(ring_offsets(ROWS)[d] + ring_offsets(COLUMNS)[r]) % 2 for d, r in offsets]
    colour = lax.rem(x + y, 2)

    def place(target, its_colour):
        return its_colour * (CHIPS // 2) + lax.div(target, 2)

    my_place = place(chip, colour)

    def owners(wanted):
        for target, is_odd in zip(all_chips, odd):
            if is_odd == wanted:
                yield target

    partner = {"seq": 2 * chip + other, "head": z}
    barrier = pltpu.get_barrier_semaphore()

    def tell(sem, target):
        pl.semaphore_signal(sem, inc=1, device_id=target, device_id_type=MESH)

    with jax.named_scope("greet"):
        for target in all_chips[:-1]:
            tell(barrier, {"seq": 2 * target + 1, "head": z})

        @pl.when(core == 1)
        def _():
            tell(barrier, partner)

        for plane in range(1, stacks):

            @pl.when(plane > z)
            def _():
                tell(barrier, {"seq": 2 * chip + 1, "head": plane})

    def meet_partner():
        @pl.when(core == 0)
        def _():
            pl.semaphore_wait(barrier, 1)
            tell(met, partner)

        @pl.when(core == 1)
        def _():
            pl.semaphore_wait(met, 1)

    def meet_plane():
        @pl.when(core == 1)
        def _():
            pl.semaphore_wait(barrier, 2 * (CHIPS - 1) + 2 * z)
            tell(met, partner)
            for plane in range(stacks - 1):

                @pl.when(plane < z)
                def _():
                    tell(stack_ready, {"seq": 2 * chip, "head": plane})
                    tell(stack_ready, {"seq": 2 * chip + 1, "head": plane})

        @pl.when(core == 0)
        def _():
            pl.semaphore_wait(met, 1)

    with jax.named_scope("load_rest"):
        for a in (1, 2):
            load(a, True).start()
        for a in (0, 3):
            load(a, False).start()
            load(a, True).start()
        load_gain.start()

    def remote(src, dst, send, recv, device):
        return pltpu.make_async_remote_copy(
            src_ref=src, dst_ref=dst, send_sem=send, recv_sem=recv, device_id=device, device_id_type=MESH
        )

    def to_core(src, dst, sent, received):
        return remote(src, dst, core_send.at[sent], core_recv.at[received], partner)

    def go(s, chunk):
        for first in range(2):

            @pl.when(colour == first)
            def _():
                for head in range(2):
                    for target in owners((head + first) % 2):
                        remote(
                            state.at[s, chunk, place(target, head)], gathered.at[s, chunk, chip],
                            go_send, go_recv.at[s, chunk], {"seq": 2 * target + other, "head": z},
                        ).start()

    def back(s, chunk):
        for target in all_chips:
            remote(
                scanned.at[s, chunk, target], prefix.at[s, chunk, my_place],
                back_send, back_recv.at[s, chunk, colour], {"seq": 2 * target + other, "head": z},
            ).start()

    def scan_back(s, chunk, reverse):
        with jax.named_scope(f"go_wait{s}{chunk}"):
            remote(gathered.at[s, chunk], gathered.at[s, chunk], go_send, go_recv.at[s, chunk], partner).wait_recv()
        with jax.named_scope(f"scan{s}{chunk}"):
            so_far = jnp.zeros((piece, HEAD_DIM), F32)
            for p in reversed(range(CHIPS)) if reverse else range(CHIPS):
                scanned[s, chunk, p] = so_far
                so_far = so_far + gathered[s, chunk, p]
        with jax.named_scope(f"back_start{s}{chunk}"):
            back(s, chunk)

    def scan_in(s, j):
        half = prefix.at[s, j // 2, pl.ds(j % 2 * (CHIPS // 2), CHIPS // 2)]
        with jax.named_scope(f"back_wait{s}{j}"):
            remote(half, half, back_send, back_recv.at[s, j // 2, j % 2], partner).wait_recv()

    def head_of(s, j):
        at = pl.ds(j % per_chunk * per_head, per_head)
        return prefix[s, j // per_chunk, at].reshape(HEAD_DIM, HEAD_DIM)

    def put_state(s, j, value):
        at = pl.ds(j % per_chunk * per_head, per_head)
        state[s, j // per_chunk, at] = value.reshape(per_head, piece, HEAD_DIM)

    def give_states(chunk):
        at = pl.ds(chunk * per_chunk, per_chunk)
        return to_core(state_out.at[at], blocks.at[core, at], 0, chunk)

    def take_states(chunk):
        at = pl.ds(chunk * per_chunk, per_chunk)
        return to_core(state_out.at[at], blocks.at[other, at], 0, chunk)

    def part_states(chunk):
        for j in heads_of(chunk):
            state_out[j] = dot(part[1, :, col(j)], part[2, :, col(j)], (0, 0))

    with jax.named_scope("load_wait"):
        for a in (1, 2):
            load(a, False).wait()
    with jax.named_scope("states_a"):
        part_states(0)
    with jax.named_scope("meet_partner"):
        meet_partner()
    give_states(0).start()
    for chunk in range(1, CHUNKS):
        part_states(chunk)
        give_states(chunk).start()
    with jax.named_scope("states_b"):
        for a in (1, 2):
            load(a, True).wait()
        for j in range(heads):
            blocks[core, j] = dot(tok[1, core, :, col(j)], tok[2, core, :, col(j)], (0, 0))
    with jax.named_scope("core_wait"):
        for chunk in range(CHUNKS):
            take_states(chunk).wait_recv()
            for j in heads_of(chunk):
                put_state(0, j, blocks[0, j] + blocks[1, j])
    with jax.named_scope("barrier"):
        meet_plane()
    for chunk in range(CHUNKS):
        with jax.named_scope(f"go0{chunk}"):
            go(0, chunk)

    causal = lax.broadcasted_iota(jnp.int32, (tokens, tokens), 0) >= lax.broadcasted_iota(
        jnp.int32, (tokens, tokens), 1
    )

    def masked(product):
        return jnp.where(causal, product * scale, 0.0).astype(BF16)

    def gain_of(j):
        return gain[pl.ds(core * heads + j, 1), :]

    def within_block(b):
        for j in range(heads):
            w = masked(dot(tok[0, b, :, col(j)], tok[1, b, :, col(j)], (1, 1)))
            weights[b, :, col(j)] = w
            attended[b, :, col(j)] = dot(w, tok[2, b, :, col(j)], (1, 0))

    with jax.named_scope("within_own"):
        load(0, True).wait()
        load(3, True).wait()
        load_gain.wait()
        for j in range(heads):
            scaled[core, :, col(j)] = cot_own[:, col(j)].astype(F32) * gain_of(j)
        within_block(core)
    def give_tokens(n):
        return to_core(stage.at[n], came.at[n], 1, CHUNKS)

    with jax.named_scope("stage"):
        for n, a in enumerate((1, 2, 0)):
            if a == 0:
                load(0, False).wait()
            stage[n] = part[a].astype(F32)
            give_tokens(n).start()
        load(3, False).wait()
        stage[3] = cot_part[...].astype(F32)
        give_tokens(3).start()

    for chunk in range(CHUNKS):
        scan_back(0, chunk, False)

    with jax.named_scope("within_other"):
        to_core(stage, came, 1, CHUNKS).wait_recv()
        for n, a in enumerate((1, 2, 0)):
            tok[a, other] = came[n].astype(BF16)
        for j in range(heads):
            scaled[other, :, col(j)] = came[3, :, col(j)] * gain_of(j)
        within_block(other)


    squares = [jnp.zeros((tokens, HEAD_DIM), F32) for _ in range(2)]
    crosses = [jnp.zeros((tokens, HEAD_DIM), F32) for _ in range(2)]
    for head in range(heads):
        scan_in(0, head)
        with jax.named_scope(f"attended{head}"):
            for j in (head,):
                before = head_of(0, j)
                low[0, j] = before.astype(BF16)
                low[1, j] = (before + blocks[0, j]).astype(BF16)
                for b in range(2):
                    att = attended[b, :, col(j)] + scale * dot(tok[0, b, :, col(j)], low[b, j], (1, 0))
                    attended[b, :, col(j)] = att
                    squares[b] = squares[b] + att * att
                    crosses[b] = crosses[b] + att * scaled[b, :, col(j)]
    me = 2 * z + core
    with jax.named_scope("statsum"):
        for r, sums in enumerate(squares + crosses):
            stats[me, pl.ds(r, 1), :] = jnp.sum(sums.T, axis=0, keepdims=True)
        @pl.when(z < stacks - 1)
        def _():
            pl.semaphore_wait(stack_ready, stacks - 1 - z)

        for up in range(1, stacks):
            for there in (core, other):
                device = {"seq": 2 * chip + there, "head": lax.rem(z + up, stacks)}
                remote(stats.at[me], stats.at[me], stat_send, stat_recv, device).start()
        remote(stats.at[me], stats.at[me], stat_send, stat_recv, partner).start()
    rest = stats.at[pl.ds(0, 2 * stacks - 1)]
    all_stats = remote(rest, rest, stat_send, stat_recv, partner)
    with jax.named_scope("stat_wait"):
        all_stats.wait_recv()
    with jax.named_scope("stat_use"):
        total = stats[0]
        for p in range(1, 2 * stacks):
            total = total + stats[p]
        inverse_rms = lax.rsqrt(total[0:2] / width + EPSILON)
        cross_mean = total[2:4] * inverse_rms / width

        def down(row):
            return jnp.broadcast_to(row, (HEAD_DIM, tokens)).T

        inverse = [down(inverse_rms[b : b + 1]) for b in range(2)]
        cross = [down(cross_mean[b : b + 1]) for b in range(2)]
    for chunk in range(CHUNKS):
        with jax.named_scope(f"grads{chunk}"):
            for j in heads_of(chunk):
                sums = []
                for b in range(2):
                    normed = attended[b, :, col(j)] * inverse[b]
                    grad = ((scaled[b, :, col(j)] - normed * cross[b]) * inverse[b]).astype(BF16)
                    grads[b, :, col(j)] = grad
                    sums.append(dot(tok[0, b, :, col(j)], grad, (0, 0)))
                late[j] = sums[1]
                put_state(1, j, sums[0] + sums[1])
        with jax.named_scope(f"go1{chunk}"):
            go(1, chunk)

    def without_suffix(b):
        for j in range(heads):
            grad = grads[b, :, col(j)]
            gw = masked(dot(grad, tok[2, b, :, col(j)], (1, 1)))
            grad_f32[0, b, :, col(j)] = dot(gw, tok[1, b, :, col(j)], (1, 0)) + scale * dot(
                grad, low[b, j], (1, 1)
            )
            grad_f32[1, b, :, col(j)] = dot(gw, tok[0, b, :, col(j)], (0, 0))
            grad_f32[2, b, :, col(j)] = dot(weights[b, :, col(j)], grad, (0, 0))

    give_query = to_core(grad_f32.at[0, other], grad_came.at[0], 2, CHUNKS + 1)

    def give(n, j):
        return to_core(grad_f32.at[n, other, :, col(j)], grad_came.at[n, :, col(j)], 2, CHUNKS + 2)

    with jax.named_scope("without_suffix"):
        without_suffix(other)
        give_query.start()
        without_suffix(core)
        result[0, :, own_cols] = grad_f32[0, core].astype(BF16)
    with jax.named_scope("dq_out"):
        give_query.wait_recv()
        result[0, :, part_cols] = grad_came[0].astype(BF16)

    for chunk in range(CHUNKS):
        scan_back(1, chunk, True)

    def with_suffix(b, j, suffix):
        grad_f32[1, b, :, col(j)] += scale * dot(tok[2, b, :, col(j)], suffix, (1, 1))
        grad_f32[2, b, :, col(j)] += scale * dot(tok[1, b, :, col(j)], suffix, (1, 0))

    for j in range(heads):
        scan_in(1, j)
        with jax.named_scope(f"with_suffix{j}"):
            after = head_of(1, j)
            with_suffix(0, j, (after + late[j]).astype(BF16))
            with_suffix(1, j, after.astype(BF16))
            for n in (1, 2):
                give(n, j).start()
    with jax.named_scope("own_out"):
        for n in (1, 2):
            result[n, :, own_cols] = grad_f32[n, core].astype(BF16)

    with jax.named_scope("send_waits"):
        to_core(state_out, state_out, 0, 0).wait_send()
        to_core(stage, stage, 1, 0).wait_send()
        remote(state, state, go_send, go_recv.at[0, 0], partner).wait_send()
        remote(scanned, scanned, back_send, go_recv.at[0, 0], partner).wait_send()
        all_stats.wait_send()
    with jax.named_scope("final_core"):
        keys_values = grad_came.at[pl.ds(1, 2)]
        to_core(keys_values, keys_values, 2, CHUNKS + 2).wait_recv()
        for n in (1, 2):
            result[n, :, part_cols] = grad_came[n].astype(BF16)
        to_core(grad_came, grad_came, 2, 0).wait_send()


def write_out(result, dq_hbm, dk_hbm, dv_hbm, sems):
    copies = [
        pltpu.make_async_copy(result.at[n], out, sems.at[n]) for n, out in enumerate((dq_hbm, dk_hbm, dv_hbm))
    ]
    for copy in copies:
        copy.start()
    for copy in copies:
        copy.wait()


def per_device(stacks, queries, keys, values, cotangent, gain):
    tokens, local = queries.shape
    mine = local // 2
    heads = mine // HEAD_DIM
    piece = heads * HEAD_DIM // CHIPS // CHUNKS
    anywhere = pl.BlockSpec(memory_space=pl.ANY)
    vmem = pl.BlockSpec(memory_space=pltpu.VMEM)
    dma = pltpu.SemaphoreType.DMA
    arrays = (queries, keys, values, cotangent, gain.reshape(2 * heads, HEAD_DIM))
    result = pl.pallas_call(
        functools.partial(kernel, stacks, mine),
        out_shape=jax.ShapeDtypeStruct((3, tokens, local), BF16),
        in_specs=[pl.BlockSpec(memory_space=pltpu.HBM)] * 5,
        out_specs=vmem,
        scratch_shapes=[
            pltpu.VMEM((2 * heads, HEAD_DIM), F32),
            pltpu.VMEM((3, 2, tokens, mine), BF16),
            pltpu.VMEM((3, tokens, mine), BF16),
            pltpu.VMEM((tokens, mine), BF16),
            pltpu.VMEM((tokens, mine), BF16),
            pltpu.VMEM((4, tokens, mine), F32),
            pltpu.VMEM((4, tokens, mine), F32),
            pltpu.VMEM((2, tokens, mine), F32),
            pltpu.VMEM((2, heads, HEAD_DIM, HEAD_DIM), F32),
            pltpu.VMEM((heads, HEAD_DIM, HEAD_DIM), F32),
            pltpu.VMEM((2, CHUNKS, CHIPS, piece, HEAD_DIM), F32),
            pltpu.VMEM((2, CHUNKS, CHIPS, piece, HEAD_DIM), F32),
            pltpu.VMEM((2, CHUNKS, CHIPS, piece, HEAD_DIM), F32),
            pltpu.VMEM((2, CHUNKS, CHIPS, piece, HEAD_DIM), F32),
            pltpu.VMEM((2, heads, HEAD_DIM, HEAD_DIM), BF16),
            pltpu.VMEM((2, tokens, mine), BF16),
            pltpu.VMEM((2, tokens, mine), F32),
            pltpu.VMEM((2 * stacks, 4, tokens), F32),
            pltpu.VMEM((2, tokens, mine), BF16),
            pltpu.VMEM((heads, HEAD_DIM, HEAD_DIM), F32),
            pltpu.VMEM((3, 2, tokens, mine), F32),
            pltpu.VMEM((3, tokens, mine), F32),
            dma((9,)),
            dma((3,)), dma((CHUNKS + 3,)),
            dma, dma((2, CHUNKS)), dma, dma((2, CHUNKS, 2)),
            dma, dma,
            pltpu.SemaphoreType.REGULAR, pltpu.SemaphoreType.REGULAR,
        ],
        compiler_params=pltpu.CompilerParams(
            collective_id=0, has_side_effects=True, vmem_limit_bytes=24 * 1024 * 1024
        ),
        name="attention",
    )(*(pltpu.with_memory_space_constraint(a, pltpu.HBM) for a in arrays))
    out = jax.ShapeDtypeStruct((tokens, local), BF16)
    return pl.pallas_call(
        write_out,
        out_shape=(out, out, out),
        in_specs=[vmem],
        out_specs=(anywhere,) * 3,
        scratch_shapes=[dma((3,))],
        compiler_params=pltpu.CompilerParams(vmem_limit_bytes=4 * 1024 * 1024),
        name="write_out",
    )(result)


def solution(mesh):
    spec = P("seq", "head")
    return jax.shard_map(
        functools.partial(per_device, mesh.shape["head"]),
        mesh=mesh,
        in_specs=(spec, spec, spec, spec, P("head")),
        out_specs=(spec, spec, spec),
        check_vma=False,
    )
```

```python
import functools

import jax
import jax.numpy as jnp
from jax import lax
from jax.experimental import pallas as pl
from jax.experimental.pallas import tpu as pltpu
from jax.sharding import PartitionSpec as P

HEAD_DIM = 128
EPSILON = 1e-05
ROWS, COLUMNS = 8, 4
CHIPS = ROWS * COLUMNS
CHUNKS = 2
PARTS = 1
MESH = pl.DeviceIdType.MESH
F32, BF16 = jnp.float32, jnp.bfloat16


def dot(a, b, over):
    return lax.dot_general(a, b, ((over[:1], over[1:]), ((), ())), preferred_element_type=F32)


def ring_offsets(size):
    return sorted(range(size), key=lambda d: -min(d, size - d))


def kernel(
    stacks, mine,
    q_hbm, k_hbm, v_hbm, cot_hbm, gain_hbm,
    result,
    gain, tok, part, cot_own, cot_part, stage, came, scaled,
    blocks, state_out, state, gathered, scanned, prefix, low,
    weights, attended, stats, grads, late,
    grad_f32, grad_came,
    load_sem, core_send, core_recv, go_send, go_recv, back_send, back_recv, stat_send, stat_recv,
    met, stack_ready,
):
    seq, z = lax.axis_index("seq"), lax.axis_index("head")
    core = lax.rem(seq, 2)
    other = 1 - core
    chip = lax.div(seq, 2)
    x, y = lax.rem(chip, COLUMNS), lax.div(chip, COLUMNS)
    heads = mine // HEAD_DIM
    per_chunk = heads // CHUNKS
    scale = HEAD_DIM ** (-0.5)
    width = 2 * mine * stacks
    tokens = tok.shape[2]
    piece = state.shape[3]
    per_head = HEAD_DIM // piece

    own_cols = pl.ds(pl.multiple_of(core * mine, mine), mine)
    part_cols = pl.ds(pl.multiple_of(other * mine, mine), mine)

    def col(j):
        return pl.ds(j * HEAD_DIM, HEAD_DIM)

    def heads_of(chunk):
        return range(chunk * per_chunk, (chunk + 1) * per_chunk)

    arrays = (q_hbm, k_hbm, v_hbm, cot_hbm)

    def load(a, own):
        if a == 3:
            target = cot_own if own else cot_part
        else:
            target = tok.at[a, core] if own else part.at[a]
        return pltpu.make_async_copy(
            arrays[a].at[:, own_cols if own else part_cols], target, load_sem.at[2 * a + int(own)]
        )

    load_gain = pltpu.make_async_copy(gain_hbm, gain, load_sem.at[8])
    with jax.named_scope("load_first"):
        for a in (1, 2):
            load(a, False).start()

    down_at = [lax.rem(y + d, ROWS) * COLUMNS for d in ring_offsets(ROWS)]
    right_at = [lax.rem(x + d, COLUMNS) for d in ring_offsets(COLUMNS)]
    offsets = [(d, r) for d in range(ROWS) for r in range(COLUMNS)]
    all_chips = [down_at[d] + right_at[r] for d, r in offsets]
    odd = [(ring_offsets(ROWS)[d] + ring_offsets(COLUMNS)[r]) % 2 for d, r in offsets]
    colour = lax.rem(x + y, 2)

    def place(target, its_colour):
        return its_colour * (CHIPS // 2) + lax.div(target, 2)

    my_place = place(chip, colour)

    def owners(wanted):
        for target, is_odd in zip(all_chips, odd):
            if is_odd == wanted:
                yield target

    partner = {"seq": 2 * chip + other, "head": z}
    barrier = pltpu.get_barrier_semaphore()

    def tell(sem, target):
        pl.semaphore_signal(sem, inc=1, device_id=target, device_id_type=MESH)

    with jax.named_scope("greet"):
        for target in all_chips[:-1]:
            tell(barrier, {"seq": 2 * target + 1, "head": z})

        @pl.when(core == 1)
        def _():
            tell(barrier, partner)

        for plane in range(1, stacks):

            @pl.when(plane > z)
            def _():
                tell(barrier, {"seq": 2 * chip + 1, "head": plane})

    def meet_partner():
        @pl.when(core == 0)
        def _():
            pl.semaphore_wait(barrier, 1)
            tell(met, partner)

        @pl.when(core == 1)
        def _():
            pl.semaphore_wait(met, 1)

    def meet_plane():
        @pl.when(core == 1)
        def _():
            pl.semaphore_wait(barrier, 2 * (CHIPS - 1) + 2 * z)
            tell(met, partner)

        @pl.when(core == 0)
        def _():
            pl.semaphore_wait(met, 1)

    with jax.named_scope("load_rest"):
        for a in (1, 2):
            load(a, True).start()
        for a in (0, 3):
            load(a, False).start()
            load(a, True).start()
        load_gain.start()

    def remote(src, dst, send, recv, device):
        return pltpu.make_async_remote_copy(
            src_ref=src, dst_ref=dst, send_sem=send, recv_sem=recv, device_id=device, device_id_type=MESH
        )

    def to_core(src, dst, sent, received):
        return remote(src, dst, core_send.at[sent], core_recv.at[received], partner)

    def go(s, j):
        chunk, head = j // 2, j % 2
        for mine_owns in range(2):

            @pl.when((colour == head) == bool(mine_owns))
            def _():
                for target in owners(1 - mine_owns):
                    remote(
                        state.at[s, chunk, place(target, head)], gathered.at[s, chunk, chip],
                        go_send, go_recv.at[s, chunk], {"seq": 2 * target + other, "head": z},
                    ).start()

    def back(s, chunk):
        def to(target):
            remote(
                scanned.at[s, chunk, target], prefix.at[s, chunk, my_place],
                back_send, back_recv.at[s, chunk, colour], {"seq": 2 * target + other, "head": z},
            ).start()

        if s == 0:
            for target in all_chips:
                to(target)
        else:
            to(0 * chip)
            for target in all_chips:
                pl.when(target != 0)(functools.partial(to, target))

    def scan_back(s, chunk, reverse):
        with jax.named_scope(f"go_wait{s}{chunk}"):
            remote(gathered.at[s, chunk], gathered.at[s, chunk], go_send, go_recv.at[s, chunk], partner).wait_recv()
        with jax.named_scope(f"scan{s}{chunk}"):
            so_far = jnp.zeros((piece, HEAD_DIM), F32)
            for p in reversed(range(CHIPS)) if reverse else range(CHIPS):
                scanned[s, chunk, p] = so_far
                so_far = so_far + gathered[s, chunk, p]
        with jax.named_scope(f"back_start{s}{chunk}"):
            back(s, chunk)

    def scan_in(s, j):
        half = prefix.at[s, j // 2, pl.ds(j % 2 * (CHIPS // 2), CHIPS // 2)]
        with jax.named_scope(f"back_wait{s}{j}"):
            remote(half, half, back_send, back_recv.at[s, j // 2, j % 2], partner).wait_recv()

    def head_of(s, j):
        at = pl.ds(j % per_chunk * per_head, per_head)
        return prefix[s, j // per_chunk, at].reshape(HEAD_DIM, HEAD_DIM)

    def put_state(s, j, value):
        at = pl.ds(j % per_chunk * per_head, per_head)
        state[s, j // per_chunk, at] = value.reshape(per_head, piece, HEAD_DIM)

    def give_states(chunk):
        at = pl.ds(chunk * per_chunk, per_chunk)
        return to_core(state_out.at[at], blocks.at[core, at], 0, chunk)

    def take_states(chunk):
        at = pl.ds(chunk * per_chunk, per_chunk)
        return to_core(state_out.at[at], blocks.at[other, at], 0, chunk)

    def part_states(chunk):
        for j in heads_of(chunk):
            state_out[j] = dot(part[1, :, col(j)], part[2, :, col(j)], (0, 0))

    with jax.named_scope("load_wait"):
        for a in (1, 2):
            load(a, False).wait()
    with jax.named_scope("states_a"):
        part_states(0)
    with jax.named_scope("meet_partner"):
        meet_partner()
    give_states(0).start()
    for chunk in range(1, CHUNKS):
        part_states(chunk)
        give_states(chunk).start()
    with jax.named_scope("states_b"):
        for a in (1, 2):
            load(a, True).wait()
        for j in range(heads):
            blocks[core, j] = dot(tok[1, core, :, col(j)], tok[2, core, :, col(j)], (0, 0))
    with jax.named_scope("core_wait"):
        for chunk in range(CHUNKS):
            take_states(chunk).wait_recv()
            for j in heads_of(chunk):
                put_state(0, j, blocks[0, j] + blocks[1, j])
    with jax.named_scope("barrier"):
        meet_plane()
    with jax.named_scope("go0"):
        for j in range(heads):
            go(0, j)

    @pl.when(core == 1)
    def _():
        for plane in range(stacks - 1):

            @pl.when(plane < z)
            def _():
                tell(stack_ready, {"seq": 2 * chip, "head": plane})
                tell(stack_ready, {"seq": 2 * chip + 1, "head": plane})

    causal = lax.broadcasted_iota(jnp.int32, (tokens, tokens), 0) >= lax.broadcasted_iota(
        jnp.int32, (tokens, tokens), 1
    )

    def masked(product):
        return jnp.where(causal, product * scale, 0.0).astype(BF16)

    def gain_of(j):
        return gain[pl.ds(core * heads + j, 1), :]

    def within_block(b):
        for j in range(heads):
            w = masked(dot(tok[0, b, :, col(j)], tok[1, b, :, col(j)], (1, 1)))
            weights[b, :, col(j)] = w
            attended[b, :, col(j)] = dot(w, tok[2, b, :, col(j)], (1, 0))

    with jax.named_scope("within_own"):
        load(0, True).wait()
        load(3, True).wait()
        load_gain.wait()
        for j in range(heads):
            scaled[core, :, col(j)] = cot_own[:, col(j)].astype(F32) * gain_of(j)
        within_block(core)
    def give_tokens(n):
        return to_core(stage.at[n], came.at[n], 1, CHUNKS)

    with jax.named_scope("stage"):
        for n, a in enumerate((1, 2, 0)):
            if a == 0:
                load(0, False).wait()
            stage[n] = part[a].astype(F32)
            give_tokens(n).start()
        load(3, False).wait()
        stage[3] = cot_part[...].astype(F32)
        give_tokens(3).start()

    for chunk in range(CHUNKS):
        scan_back(0, chunk, False)

    with jax.named_scope("within_other"):
        to_core(stage, came, 1, CHUNKS).wait_recv()
        for n, a in enumerate((1, 2, 0)):
            tok[a, other] = came[n].astype(BF16)
        for j in range(heads):
            scaled[other, :, col(j)] = came[3, :, col(j)] * gain_of(j)
        within_block(other)


    squares = [jnp.zeros((tokens, HEAD_DIM), F32) for _ in range(2)]
    crosses = [jnp.zeros((tokens, HEAD_DIM), F32) for _ in range(2)]
    for head in range(heads):
        scan_in(0, head)
        with jax.named_scope(f"attended{head}"):
            for j in (head,):
                before = head_of(0, j)
                low[0, j] = before.astype(BF16)
                low[1, j] = (before + blocks[0, j]).astype(BF16)
                for b in range(2):
                    att = attended[b, :, col(j)] + scale * dot(tok[0, b, :, col(j)], low[b, j], (1, 0))
                    attended[b, :, col(j)] = att
                    squares[b] = squares[b] + att * att
                    crosses[b] = crosses[b] + att * scaled[b, :, col(j)]
    me = 2 * z + core
    with jax.named_scope("statsum"):
        for r, sums in enumerate(squares + crosses):
            stats[me, pl.ds(r, 1), :] = jnp.sum(sums.T, axis=0, keepdims=True)
        @pl.when(z < stacks - 1)
        def _():
            pl.semaphore_wait(stack_ready, stacks - 1 - z)

        for up in range(1, stacks):
            for there in (core, other):
                device = {"seq": 2 * chip + there, "head": lax.rem(z + up, stacks)}
                remote(stats.at[me], stats.at[me], stat_send, stat_recv, device).start()
        remote(stats.at[me], stats.at[me], stat_send, stat_recv, partner).start()
    rest = stats.at[pl.ds(0, 2 * stacks - 1)]
    all_stats = remote(rest, rest, stat_send, stat_recv, partner)
    with jax.named_scope("stat_wait"):
        all_stats.wait_recv()
    with jax.named_scope("stat_use"):
        total = stats[0]
        for p in range(1, 2 * stacks):
            total = total + stats[p]
        inverse_rms = lax.rsqrt(total[0:2] / width + EPSILON)
        cross_mean = total[2:4] * inverse_rms / width

        def down(row):
            return jnp.broadcast_to(row, (HEAD_DIM, tokens)).T

        inverse = [down(inverse_rms[b : b + 1]) for b in range(2)]
        cross = [down(cross_mean[b : b + 1]) for b in range(2)]
    for j in range(heads):
        with jax.named_scope(f"grads{j}"):
            sums = []
            for b in range(2):
                normed = attended[b, :, col(j)] * inverse[b]
                grad = ((scaled[b, :, col(j)] - normed * cross[b]) * inverse[b]).astype(BF16)
                grads[b, :, col(j)] = grad
                sums.append(dot(tok[0, b, :, col(j)], grad, (0, 0)))
            late[j] = sums[1]
            put_state(1, j, sums[0] + sums[1])
            go(1, j)

    def without_suffix(b):
        for j in range(heads):
            grad = grads[b, :, col(j)]
            gw = masked(dot(grad, tok[2, b, :, col(j)], (1, 1)))
            grad_f32[0, b, :, col(j)] = dot(gw, tok[1, b, :, col(j)], (1, 0)) + scale * dot(
                grad, low[b, j], (1, 1)
            )
            grad_f32[1, b, :, col(j)] = dot(gw, tok[0, b, :, col(j)], (0, 0))
            grad_f32[2, b, :, col(j)] = dot(weights[b, :, col(j)], grad, (0, 0))

    give_query = to_core(grad_f32.at[0, other], grad_came.at[0], 2, CHUNKS + 1)

    def give(n, j):
        return to_core(grad_f32.at[n, other, :, col(j)], grad_came.at[n, :, col(j)], 2, CHUNKS + 2)

    with jax.named_scope("without_suffix"):
        without_suffix(other)
        give_query.start()
        without_suffix(core)
        result[0, :, own_cols] = grad_f32[0, core].astype(BF16)
    with jax.named_scope("dq_out"):
        give_query.wait_recv()
        result[0, :, part_cols] = grad_came[0].astype(BF16)

    for chunk in range(CHUNKS):
        scan_back(1, chunk, True)

    def with_suffix(b, j, suffix):
        grad_f32[1, b, :, col(j)] += scale * dot(tok[2, b, :, col(j)], suffix, (1, 1))
        grad_f32[2, b, :, col(j)] += scale * dot(tok[1, b, :, col(j)], suffix, (1, 0))

    for j in range(heads):
        scan_in(1, j)
        with jax.named_scope(f"with_suffix{j}"):
            after = head_of(1, j)
            with_suffix(0, j, (after + late[j]).astype(BF16))
            with_suffix(1, j, after.astype(BF16))
            for n in (1, 2):
                give(n, j).start()
    with jax.named_scope("own_out"):
        for n in (1, 2):
            result[n, :, own_cols] = grad_f32[n, core].astype(BF16)

    with jax.named_scope("send_waits"):
        to_core(state_out, state_out, 0, 0).wait_send()
        to_core(stage, stage, 1, 0).wait_send()
        remote(state, state, go_send, go_recv.at[0, 0], partner).wait_send()
        remote(scanned, scanned, back_send, go_recv.at[0, 0], partner).wait_send()
        all_stats.wait_send()
    with jax.named_scope("final_core"):
        keys_values = grad_came.at[pl.ds(1, 2)]
        to_core(keys_values, keys_values, 2, CHUNKS + 2).wait_recv()
        for n in (1, 2):
            result[n, :, part_cols] = grad_came[n].astype(BF16)
        to_core(grad_came, grad_came, 2, 0).wait_send()


def write_out(result, dq_hbm, dk_hbm, dv_hbm, sems):
    step = result.shape[1] // PARTS
    copies = [
        pltpu.make_async_copy(
            result.at[n, pl.ds(p * step, step)], out.at[pl.ds(p * step, step)], sems.at[PARTS * n + p]
        )
        for n, out in enumerate((dq_hbm, dk_hbm, dv_hbm))
        for p in range(PARTS)
    ]
    for copy in copies:
        copy.start()
    for copy in copies:
        copy.wait()


def per_device(stacks, queries, keys, values, cotangent, gain):
    tokens, local = queries.shape
    mine = local // 2
    heads = mine // HEAD_DIM
    piece = heads * HEAD_DIM // CHIPS // CHUNKS
    anywhere = pl.BlockSpec(memory_space=pl.ANY)
    vmem = pl.BlockSpec(memory_space=pltpu.VMEM)
    dma = pltpu.SemaphoreType.DMA
    arrays = (queries, keys, values, cotangent, gain.reshape(2 * heads, HEAD_DIM))
    result = pl.pallas_call(
        functools.partial(kernel, stacks, mine),
        out_shape=jax.ShapeDtypeStruct((3, tokens, local), BF16),
        in_specs=[pl.BlockSpec(memory_space=pltpu.HBM)] * 5,
        out_specs=vmem,
        scratch_shapes=[
            pltpu.VMEM((2 * heads, HEAD_DIM), F32),
            pltpu.VMEM((3, 2, tokens, mine), BF16),
            pltpu.VMEM((3, tokens, mine), BF16),
            pltpu.VMEM((tokens, mine), BF16),
            pltpu.VMEM((tokens, mine), BF16),
            pltpu.VMEM((4, tokens, mine), F32),
            pltpu.VMEM((4, tokens, mine), F32),
            pltpu.VMEM((2, tokens, mine), F32),
            pltpu.VMEM((2, heads, HEAD_DIM, HEAD_DIM), F32),
            pltpu.VMEM((heads, HEAD_DIM, HEAD_DIM), F32),
            pltpu.VMEM((2, CHUNKS, CHIPS, piece, HEAD_DIM), F32),
            pltpu.VMEM((2, CHUNKS, CHIPS, piece, HEAD_DIM), F32),
            pltpu.VMEM((2, CHUNKS, CHIPS, piece, HEAD_DIM), F32),
            pltpu.VMEM((2, CHUNKS, CHIPS, piece, HEAD_DIM), F32),
            pltpu.VMEM((2, heads, HEAD_DIM, HEAD_DIM), BF16),
            pltpu.VMEM((2, tokens, mine), BF16),
            pltpu.VMEM((2, tokens, mine), F32),
            pltpu.VMEM((2 * stacks, 4, tokens), F32),
            pltpu.VMEM((2, tokens, mine), BF16),
            pltpu.VMEM((heads, HEAD_DIM, HEAD_DIM), F32),
            pltpu.VMEM((3, 2, tokens, mine), F32),
            pltpu.VMEM((3, tokens, mine), F32),
            dma((9,)),
            dma((3,)), dma((CHUNKS + 3,)),
            dma, dma((2, CHUNKS)), dma, dma((2, CHUNKS, 2)),
            dma, dma,
            pltpu.SemaphoreType.REGULAR, pltpu.SemaphoreType.REGULAR,
        ],
        compiler_params=pltpu.CompilerParams(
            collective_id=0, has_side_effects=True, vmem_limit_bytes=24 * 1024 * 1024
        ),
        name="attention",
    )(*(pltpu.with_memory_space_constraint(a, pltpu.HBM) for a in arrays))
    out = jax.ShapeDtypeStruct((tokens, local), BF16)
    return pl.pallas_call(
        write_out,
        out_shape=(out, out, out),
        in_specs=[vmem],
        out_specs=(anywhere,) * 3,
        scratch_shapes=[dma((3 * PARTS,))],
        compiler_params=pltpu.CompilerParams(vmem_limit_bytes=4 * 1024 * 1024),
        name="write_out",
    )(result)


def solution(mesh):
    spec = P("seq", "head")
    return jax.shard_map(
        functools.partial(per_device, mesh.shape["head"]),
        mesh=mesh,
        in_specs=(spec, spec, spec, spec, P("head")),
        out_specs=(spec, spec, spec),
        check_vma=False,
    )
```

```python
import functools

import jax
import jax.numpy as jnp
from jax import lax
from jax.experimental import pallas as pl
from jax.experimental.pallas import tpu as pltpu
from jax.sharding import PartitionSpec as P

HEAD_DIM = 128
EPSILON = 1e-05
ROWS, COLUMNS = 8, 4
CHIPS = ROWS * COLUMNS
CHUNKS = 2
PARTS = 1
FIRST = (0,)
MESH = pl.DeviceIdType.MESH
F32, BF16 = jnp.float32, jnp.bfloat16


def dot(a, b, over):
    return lax.dot_general(a, b, ((over[:1], over[1:]), ((), ())), preferred_element_type=F32)


def ring_offsets(size):
    return sorted(range(size), key=lambda d: -min(d, size - d))


def kernel(
    stacks, mine,
    q_hbm, k_hbm, v_hbm, cot_hbm, gain_hbm,
    result,
    gain, tok, part, cot_own, cot_part, stage, came, scaled,
    blocks, state_out, state, gathered, scanned, prefix, low,
    weights, attended, stats, grads, late,
    grad_f32, grad_came, early, prefix_part,
    load_sem, core_send, core_recv, go_send, go_recv, back_send, back_recv, stat_send, stat_recv,
    met, stack_ready, twice_send, twice_recv,
):
    seq, z = lax.axis_index("seq"), lax.axis_index("head")
    core = lax.rem(seq, 2)
    other = 1 - core
    chip = lax.div(seq, 2)
    x, y = lax.rem(chip, COLUMNS), lax.div(chip, COLUMNS)
    heads = mine // HEAD_DIM
    per_chunk = heads // CHUNKS
    scale = HEAD_DIM ** (-0.5)
    width = 2 * mine * stacks
    tokens = tok.shape[2]
    piece = state.shape[3]
    per_head = HEAD_DIM // piece

    own_cols = pl.ds(pl.multiple_of(core * mine, mine), mine)
    part_cols = pl.ds(pl.multiple_of(other * mine, mine), mine)

    def col(j):
        return pl.ds(j * HEAD_DIM, HEAD_DIM)

    def heads_of(chunk):
        return range(chunk * per_chunk, (chunk + 1) * per_chunk)

    arrays = (q_hbm, k_hbm, v_hbm, cot_hbm)

    def load(a, own):
        if a == 3:
            target = cot_own if own else cot_part
        else:
            target = tok.at[a, core] if own else part.at[a]
        return pltpu.make_async_copy(
            arrays[a].at[:, own_cols if own else part_cols], target, load_sem.at[2 * a + int(own)]
        )

    load_gain = pltpu.make_async_copy(gain_hbm, gain, load_sem.at[8])
    with jax.named_scope("load_first"):
        for a in (1, 2):
            load(a, False).start()

    down_at = [lax.rem(y + d, ROWS) * COLUMNS for d in ring_offsets(ROWS)]
    right_at = [lax.rem(x + d, COLUMNS) for d in ring_offsets(COLUMNS)]
    offsets = [(d, r) for d in range(ROWS) for r in range(COLUMNS)]
    all_chips = [down_at[d] + right_at[r] for d, r in offsets]
    odd = [(ring_offsets(ROWS)[d] + ring_offsets(COLUMNS)[r]) % 2 for d, r in offsets]
    colour = lax.rem(x + y, 2)

    def place(target, its_colour):
        return its_colour * (CHIPS // 2) + lax.div(target, 2)

    my_place = place(chip, colour)

    def owners(wanted):
        for target, is_odd in zip(all_chips, odd):
            if is_odd == wanted:
                yield target

    partner = {"seq": 2 * chip + other, "head": z}
    barrier = pltpu.get_barrier_semaphore()

    def tell(sem, target):
        pl.semaphore_signal(sem, inc=1, device_id=target, device_id_type=MESH)

    with jax.named_scope("greet"):
        for target in all_chips[:-1]:
            tell(barrier, {"seq": 2 * target + 1, "head": z})

        @pl.when(core == 1)
        def _():
            tell(barrier, partner)

        for plane in range(1, stacks):

            @pl.when(plane > z)
            def _():
                tell(barrier, {"seq": 2 * chip + 1, "head": plane})

    def meet_partner():
        @pl.when(core == 0)
        def _():
            pl.semaphore_wait(barrier, 1)
            tell(met, partner)

        @pl.when(core == 1)
        def _():
            pl.semaphore_wait(met, 1)

    def meet_plane():
        @pl.when(core == 1)
        def _():
            pl.semaphore_wait(barrier, 2 * (CHIPS - 1) + 2 * z)
            tell(met, partner)

        @pl.when(core == 0)
        def _():
            pl.semaphore_wait(met, 1)

    with jax.named_scope("load_rest"):
        for a in (1, 2):
            load(a, True).start()
        for a in (0, 3):
            load(a, False).start()
            load(a, True).start()
        load_gain.start()

    def remote(src, dst, send, recv, device):
        return pltpu.make_async_remote_copy(
            src_ref=src, dst_ref=dst, send_sem=send, recv_sem=recv, device_id=device, device_id_type=MESH
        )

    def to_core(src, dst, sent, received):
        return remote(src, dst, core_send.at[sent], core_recv.at[received], partner)

    def go(s, j):
        chunk, head = j // 2, j % 2
        for mine_owns in range(2):

            @pl.when((colour == head) == bool(mine_owns))
            def _():
                for target in owners(1 - mine_owns):
                    remote(
                        state.at[s, chunk, place(target, head)], gathered.at[s, chunk, chip],
                        go_send, go_recv.at[s, chunk], {"seq": 2 * target + other, "head": z},
                    ).start()

    def back(s, chunk):
        def to(target):
            remote(
                scanned.at[s, chunk, target], prefix.at[s, chunk, my_place],
                back_send, back_recv.at[s, chunk, colour], {"seq": 2 * target + other, "head": z},
            ).start()

        def twice(target):
            @pl.when(jnp.logical_and(core == 1, chip != target))
            def _():
                remote(
                    scanned.at[s, chunk, target], prefix_part.at[chunk, my_place],
                    twice_send, twice_recv.at[chunk, colour], {"seq": 2 * target + 1 + 0 * chip, "head": z},
                ).start()

            @pl.when(jnp.logical_and(core == 1, chip == target))
            def _():
                prefix_part[chunk, my_place] = scanned[s, chunk, target]

        if s == 0:
            for target in all_chips:
                to(target)
        else:
            for target in FIRST:
                to(target + 0 * chip)
                twice(target)
            for target in all_chips:
                ahead = functools.reduce(jnp.logical_or, [target == t for t in FIRST])
                pl.when(jnp.logical_not(ahead))(functools.partial(to, target))

    def scan_back(s, chunk, reverse):
        with jax.named_scope(f"go_wait{s}{chunk}"):
            remote(gathered.at[s, chunk], gathered.at[s, chunk], go_send, go_recv.at[s, chunk], partner).wait_recv()
        with jax.named_scope(f"scan{s}{chunk}"):
            so_far = jnp.zeros((piece, HEAD_DIM), F32)
            for p in reversed(range(CHIPS)) if reverse else range(CHIPS):
                scanned[s, chunk, p] = so_far
                so_far = so_far + gathered[s, chunk, p]
        with jax.named_scope(f"back_start{s}{chunk}"):
            back(s, chunk)

    def scan_in(s, j):
        half = prefix.at[s, j // 2, pl.ds(j % 2 * (CHIPS // 2), CHIPS // 2)]
        with jax.named_scope(f"back_wait{s}{j}"):
            remote(half, half, back_send, back_recv.at[s, j // 2, j % 2], partner).wait_recv()

    def head_of(s, j):
        at = pl.ds(j % per_chunk * per_head, per_head)
        return prefix[s, j // per_chunk, at].reshape(HEAD_DIM, HEAD_DIM)

    def put_state(s, j, value):
        at = pl.ds(j % per_chunk * per_head, per_head)
        state[s, j // per_chunk, at] = value.reshape(per_head, piece, HEAD_DIM)

    def give_states(chunk):
        at = pl.ds(chunk * per_chunk, per_chunk)
        return to_core(state_out.at[at], blocks.at[core, at], 0, chunk)

    def take_states(chunk):
        at = pl.ds(chunk * per_chunk, per_chunk)
        return to_core(state_out.at[at], blocks.at[other, at], 0, chunk)

    def part_states(chunk):
        for j in heads_of(chunk):
            state_out[j] = dot(part[1, :, col(j)], part[2, :, col(j)], (0, 0))

    with jax.named_scope("load_wait"):
        for a in (1, 2):
            load(a, False).wait()
    with jax.named_scope("states_a"):
        part_states(0)
    with jax.named_scope("meet_partner"):
        meet_partner()
    give_states(0).start()
    for chunk in range(1, CHUNKS):
        part_states(chunk)
        give_states(chunk).start()
    with jax.named_scope("states_b"):
        for a in (1, 2):
            load(a, True).wait()
        for j in range(heads):
            blocks[core, j] = dot(tok[1, core, :, col(j)], tok[2, core, :, col(j)], (0, 0))
    with jax.named_scope("core_wait"):
        for chunk in range(CHUNKS):
            take_states(chunk).wait_recv()
            for j in heads_of(chunk):
                put_state(0, j, blocks[0, j] + blocks[1, j])
    with jax.named_scope("barrier"):
        meet_plane()
    with jax.named_scope("go0"):
        for j in range(heads):
            go(0, j)

    @pl.when(core == 1)
    def _():
        for plane in range(stacks - 1):

            @pl.when(plane < z)
            def _():
                tell(stack_ready, {"seq": 2 * chip, "head": plane})
                tell(stack_ready, {"seq": 2 * chip + 1, "head": plane})

    causal = lax.broadcasted_iota(jnp.int32, (tokens, tokens), 0) >= lax.broadcasted_iota(
        jnp.int32, (tokens, tokens), 1
    )

    def masked(product):
        return jnp.where(causal, product * scale, 0.0).astype(BF16)

    def gain_of(j):
        return gain[pl.ds(core * heads + j, 1), :]

    def within_block(b):
        for j in range(heads):
            w = masked(dot(tok[0, b, :, col(j)], tok[1, b, :, col(j)], (1, 1)))
            weights[b, :, col(j)] = w
            attended[b, :, col(j)] = dot(w, tok[2, b, :, col(j)], (1, 0))

    with jax.named_scope("within_own"):
        load(0, True).wait()
        load(3, True).wait()
        load_gain.wait()
        for j in range(heads):
            scaled[core, :, col(j)] = cot_own[:, col(j)].astype(F32) * gain_of(j)
        within_block(core)
    def give_tokens(n):
        return to_core(stage.at[n], came.at[n], 1, CHUNKS)

    with jax.named_scope("stage"):
        for n, a in enumerate((1, 2, 0)):
            if a == 0:
                load(0, False).wait()
            stage[n] = part[a].astype(F32)
            give_tokens(n).start()
        load(3, False).wait()
        stage[3] = cot_part[...].astype(F32)
        give_tokens(3).start()

    for chunk in range(CHUNKS):
        scan_back(0, chunk, False)

    with jax.named_scope("within_other"):
        to_core(stage, came, 1, CHUNKS).wait_recv()
        for n, a in enumerate((1, 2, 0)):
            tok[a, other] = came[n].astype(BF16)
        for j in range(heads):
            scaled[other, :, col(j)] = came[3, :, col(j)] * gain_of(j)
        within_block(other)


    squares = [jnp.zeros((tokens, HEAD_DIM), F32) for _ in range(2)]
    crosses = [jnp.zeros((tokens, HEAD_DIM), F32) for _ in range(2)]
    for head in range(heads):
        scan_in(0, head)
        with jax.named_scope(f"attended{head}"):
            for j in (head,):
                before = head_of(0, j)
                low[0, j] = before.astype(BF16)
                low[1, j] = (before + blocks[0, j]).astype(BF16)
                for b in range(2):
                    att = attended[b, :, col(j)] + scale * dot(tok[0, b, :, col(j)], low[b, j], (1, 0))
                    attended[b, :, col(j)] = att
                    squares[b] = squares[b] + att * att
                    crosses[b] = crosses[b] + att * scaled[b, :, col(j)]
    me = 2 * z + core
    with jax.named_scope("statsum"):
        for r, sums in enumerate(squares + crosses):
            stats[me, pl.ds(r, 1), :] = jnp.sum(sums.T, axis=0, keepdims=True)
        @pl.when(z < stacks - 1)
        def _():
            pl.semaphore_wait(stack_ready, stacks - 1 - z)

        for up in range(1, stacks):
            for there in (core, other):
                device = {"seq": 2 * chip + there, "head": lax.rem(z + up, stacks)}
                remote(stats.at[me], stats.at[me], stat_send, stat_recv, device).start()
        remote(stats.at[me], stats.at[me], stat_send, stat_recv, partner).start()
    rest = stats.at[pl.ds(0, 2 * stacks - 1)]
    all_stats = remote(rest, rest, stat_send, stat_recv, partner)
    with jax.named_scope("stat_wait"):
        all_stats.wait_recv()
    with jax.named_scope("stat_use"):
        total = stats[0]
        for p in range(1, 2 * stacks):
            total = total + stats[p]
        inverse_rms = lax.rsqrt(total[0:2] / width + EPSILON)
        cross_mean = total[2:4] * inverse_rms / width

        def down(row):
            return jnp.broadcast_to(row, (HEAD_DIM, tokens)).T

        inverse = [down(inverse_rms[b : b + 1]) for b in range(2)]
        cross = [down(cross_mean[b : b + 1]) for b in range(2)]
    for j in range(heads):
        with jax.named_scope(f"grads{j}"):
            sums = []
            for b in range(2):
                normed = attended[b, :, col(j)] * inverse[b]
                grad = ((scaled[b, :, col(j)] - normed * cross[b]) * inverse[b]).astype(BF16)
                grads[b, :, col(j)] = grad
                sums.append(dot(tok[0, b, :, col(j)], grad, (0, 0)))
            late[j] = sums[1]
            put_state(1, j, sums[0] + sums[1])
            go(1, j)

    def without_suffix(b):
        for j in range(heads):
            grad = grads[b, :, col(j)]
            gw = masked(dot(grad, tok[2, b, :, col(j)], (1, 1)))
            grad_f32[0, b, :, col(j)] = dot(gw, tok[1, b, :, col(j)], (1, 0)) + scale * dot(
                grad, low[b, j], (1, 1)
            )
            grad_f32[1, b, :, col(j)] = dot(gw, tok[0, b, :, col(j)], (0, 0))
            grad_f32[2, b, :, col(j)] = dot(weights[b, :, col(j)], grad, (0, 0))

    give_query = to_core(grad_f32.at[0, other], grad_came.at[0], 2, CHUNKS + 1)

    def give(n, j):
        return to_core(grad_f32.at[n, other, :, col(j)], grad_came.at[n, :, col(j)], 2, CHUNKS + 2)

    keys_values = grad_came.at[pl.ds(1, 2)]
    give_early = to_core(early, keys_values, 2, CHUNKS + 2)
    is_first = functools.reduce(jnp.logical_or, [chip == t for t in FIRST])
    with jax.named_scope("without_suffix"):
        without_suffix(other)
        give_query.start()

        @pl.when(jnp.logical_and(is_first, core == 0))
        def _():
            for n in (1, 2):
                early[n - 1] = grad_f32[n, 1]
            give_early.start()

        without_suffix(core)
        result[0, :, own_cols] = grad_f32[0, core].astype(BF16)
    with jax.named_scope("dq_out"):
        give_query.wait_recv()
        result[0, :, part_cols] = grad_came[0].astype(BF16)

    for chunk in range(CHUNKS):
        scan_back(1, chunk, True)

    def with_suffix(b, j, suffix):
        grad_f32[1, b, :, col(j)] += scale * dot(tok[2, b, :, col(j)], suffix, (1, 1))
        grad_f32[2, b, :, col(j)] += scale * dot(tok[1, b, :, col(j)], suffix, (1, 0))

    for j in range(heads):
        scan_in(1, j)
        with jax.named_scope(f"with_suffix{j}"):
            after = head_of(1, j)
            with_suffix(0, j, (after + late[j]).astype(BF16))
            with_suffix(1, j, after.astype(BF16))

            @pl.when(jnp.logical_not(jnp.logical_and(is_first, core == 0)))
            def _():
                for n in (1, 2):
                    give(n, j).start()

    with jax.named_scope("own_out"):
        for n in (1, 2):
            result[n, :, own_cols] = grad_f32[n, core].astype(BF16)

    with jax.named_scope("send_waits"):
        to_core(state_out, state_out, 0, 0).wait_send()
        to_core(stage, stage, 1, 0).wait_send()
        remote(state, state, go_send, go_recv.at[0, 0], partner).wait_send()
        remote(scanned, scanned, back_send, go_recv.at[0, 0], partner).wait_send()
        all_stats.wait_send()
    with jax.named_scope("final_core"):
        to_core(keys_values, keys_values, 2, CHUNKS + 2).wait_recv()

        @pl.when(jnp.logical_not(jnp.logical_and(is_first, core == 1)))
        def _():
            for n in (1, 2):
                result[n, :, part_cols] = grad_came[n].astype(BF16)

        @pl.when(jnp.logical_and(is_first, core == 1))
        def _():
            for j in range(heads):
                chunk, head = divmod(j, 2)
                for own in range(2):

                    @pl.when((colour == head) == bool(own))
                    def _():
                        pieces = prefix_part.at[chunk, pl.ds(head * (CHIPS // 2), CHIPS // 2 - own)]
                        remote(pieces, pieces, twice_send, twice_recv.at[chunk, head], partner).wait_recv()

            for j in range(heads):
                at = pl.ds(j % per_chunk * per_head, per_head)
                suffix = prefix_part[j // per_chunk, at].reshape(HEAD_DIM, HEAD_DIM).astype(BF16)
                cols = pl.ds(pl.multiple_of(other * mine + j * HEAD_DIM, HEAD_DIM), HEAD_DIM)
                keys = grad_came[1, :, col(j)] + scale * dot(part[2, :, col(j)], suffix, (1, 1))
                values = grad_came[2, :, col(j)] + scale * dot(part[1, :, col(j)], suffix, (1, 0))
                result[1, :, cols] = keys.astype(BF16)
                result[2, :, cols] = values.astype(BF16)

        to_core(grad_came, grad_came, 2, 0).wait_send()
        for own in range(2):
            count = CHUNKS * (len(FIRST) - own)
            if count:

                @pl.when(jnp.logical_and(core == 1, is_first == bool(own)))
                def _():
                    pieces = scanned.at[1, 0, pl.ds(0, count)]
                    remote(pieces, pieces, twice_send, twice_recv.at[0, 0], partner).wait_send()


def write_out(result, dq_hbm, dk_hbm, dv_hbm, sems):
    step = result.shape[1] // PARTS
    copies = [
        pltpu.make_async_copy(
            result.at[n, pl.ds(p * step, step)], out.at[pl.ds(p * step, step)], sems.at[PARTS * n + p]
        )
        for n, out in enumerate((dq_hbm, dk_hbm, dv_hbm))
        for p in range(PARTS)
    ]
    for copy in copies:
        copy.start()
    for copy in copies:
        copy.wait()


def per_device(stacks, queries, keys, values, cotangent, gain):
    tokens, local = queries.shape
    mine = local // 2
    heads = mine // HEAD_DIM
    piece = heads * HEAD_DIM // CHIPS // CHUNKS
    anywhere = pl.BlockSpec(memory_space=pl.ANY)
    vmem = pl.BlockSpec(memory_space=pltpu.VMEM)
    dma = pltpu.SemaphoreType.DMA
    arrays = (queries, keys, values, cotangent, gain.reshape(2 * heads, HEAD_DIM))
    result = pl.pallas_call(
        functools.partial(kernel, stacks, mine),
        out_shape=jax.ShapeDtypeStruct((3, tokens, local), BF16),
        in_specs=[pl.BlockSpec(memory_space=pltpu.HBM)] * 5,
        out_specs=vmem,
        scratch_shapes=[
            pltpu.VMEM((2 * heads, HEAD_DIM), F32),
            pltpu.VMEM((3, 2, tokens, mine), BF16),
            pltpu.VMEM((3, tokens, mine), BF16),
            pltpu.VMEM((tokens, mine), BF16),
            pltpu.VMEM((tokens, mine), BF16),
            pltpu.VMEM((4, tokens, mine), F32),
            pltpu.VMEM((4, tokens, mine), F32),
            pltpu.VMEM((2, tokens, mine), F32),
            pltpu.VMEM((2, heads, HEAD_DIM, HEAD_DIM), F32),
            pltpu.VMEM((heads, HEAD_DIM, HEAD_DIM), F32),
            pltpu.VMEM((2, CHUNKS, CHIPS, piece, HEAD_DIM), F32),
            pltpu.VMEM((2, CHUNKS, CHIPS, piece, HEAD_DIM), F32),
            pltpu.VMEM((2, CHUNKS, CHIPS, piece, HEAD_DIM), F32),
            pltpu.VMEM((2, CHUNKS, CHIPS, piece, HEAD_DIM), F32),
            pltpu.VMEM((2, heads, HEAD_DIM, HEAD_DIM), BF16),
            pltpu.VMEM((2, tokens, mine), BF16),
            pltpu.VMEM((2, tokens, mine), F32),
            pltpu.VMEM((2 * stacks, 4, tokens), F32),
            pltpu.VMEM((2, tokens, mine), BF16),
            pltpu.VMEM((heads, HEAD_DIM, HEAD_DIM), F32),
            pltpu.VMEM((3, 2, tokens, mine), F32),
            pltpu.VMEM((3, tokens, mine), F32),
            pltpu.VMEM((2, tokens, mine), F32),
            pltpu.VMEM((CHUNKS, CHIPS, piece, HEAD_DIM), F32),
            dma((9,)),
            dma((3,)), dma((CHUNKS + 3,)),
            dma, dma((2, CHUNKS)), dma, dma((2, CHUNKS, 2)),
            dma, dma,
            pltpu.SemaphoreType.REGULAR, pltpu.SemaphoreType.REGULAR,
            dma, dma((CHUNKS, 2)),
        ],
        compiler_params=pltpu.CompilerParams(
            collective_id=0, has_side_effects=True, vmem_limit_bytes=24 * 1024 * 1024
        ),
        name="attention",
    )(*(pltpu.with_memory_space_constraint(a, pltpu.HBM) for a in arrays))
    out = jax.ShapeDtypeStruct((tokens, local), BF16)
    return pl.pallas_call(
        write_out,
        out_shape=(out, out, out),
        in_specs=[vmem],
        out_specs=(anywhere,) * 3,
        scratch_shapes=[dma((3 * PARTS,))],
        compiler_params=pltpu.CompilerParams(vmem_limit_bytes=4 * 1024 * 1024),
        name="write_out",
    )(result)


def solution(mesh):
    spec = P("seq", "head")
    return jax.shard_map(
        functools.partial(per_device, mesh.shape["head"]),
        mesh=mesh,
        in_specs=(spec, spec, spec, spec, P("head")),
        out_specs=(spec, spec, spec),
        check_vma=False,
    )
```

```python
import functools

import jax
import jax.numpy as jnp
from jax import lax
from jax.experimental import pallas as pl
from jax.experimental.pallas import tpu as pltpu
from jax.sharding import PartitionSpec as P

HEAD_DIM = 128
EPSILON = 1e-05
ROWS, COLUMNS = 8, 4
CHIPS = ROWS * COLUMNS
CHUNKS = 2
PARTS = 1
MESH = pl.DeviceIdType.MESH
F32, BF16 = jnp.float32, jnp.bfloat16


def dot(a, b, over):
    return lax.dot_general(a, b, ((over[:1], over[1:]), ((), ())), preferred_element_type=F32)


def ring_offsets(size):
    return sorted(range(size), key=lambda d: -min(d, size - d))


def kernel(
    stacks, mine,
    q_hbm, k_hbm, v_hbm, cot_hbm, gain_hbm,
    result,
    gain, tok, part, cot_own, cot_part, stage, came, scaled,
    blocks, state_out, state, gathered, scanned, prefix, low,
    weights, attended, stats, grads, late,
    grad_f32, grad_came, early, prefix_part,
    load_sem, core_send, core_recv, go_send, go_recv, back_send, back_recv, stat_send, stat_recv,
    met, stack_ready, twice_send, twice_recv,
):
    seq, z = lax.axis_index("seq"), lax.axis_index("head")
    core = lax.rem(seq, 2)
    other = 1 - core
    chip = lax.div(seq, 2)
    x, y = lax.rem(chip, COLUMNS), lax.div(chip, COLUMNS)
    heads = mine // HEAD_DIM
    per_chunk = heads // CHUNKS
    scale = HEAD_DIM ** (-0.5)
    width = 2 * mine * stacks
    tokens = tok.shape[2]
    piece = state.shape[3]
    per_head = HEAD_DIM // piece

    own_cols = pl.ds(pl.multiple_of(core * mine, mine), mine)
    part_cols = pl.ds(pl.multiple_of(other * mine, mine), mine)

    def col(j):
        return pl.ds(j * HEAD_DIM, HEAD_DIM)

    def heads_of(chunk):
        return range(chunk * per_chunk, (chunk + 1) * per_chunk)

    arrays = (q_hbm, k_hbm, v_hbm, cot_hbm)

    def load(a, own):
        if a == 3:
            target = cot_own if own else cot_part
        else:
            target = tok.at[a, core] if own else part.at[a]
        return pltpu.make_async_copy(
            arrays[a].at[:, own_cols if own else part_cols], target, load_sem.at[2 * a + int(own)]
        )

    load_gain = pltpu.make_async_copy(gain_hbm, gain, load_sem.at[8])
    with jax.named_scope("load_first"):
        for a in (1, 2):
            load(a, False).start()

    down_at = [lax.rem(y + d, ROWS) * COLUMNS for d in ring_offsets(ROWS)]
    right_at = [lax.rem(x + d, COLUMNS) for d in ring_offsets(COLUMNS)]
    offsets = [(d, r) for d in range(ROWS) for r in range(COLUMNS)]
    all_chips = [down_at[d] + right_at[r] for d, r in offsets]
    odd = [(ring_offsets(ROWS)[d] + ring_offsets(COLUMNS)[r]) % 2 for d, r in offsets]
    colour = lax.rem(x + y, 2)

    def place(target, its_colour):
        return its_colour * (CHIPS // 2) + lax.div(target, 2)

    my_place = place(chip, colour)

    def owners(wanted):
        for target, is_odd in zip(all_chips, odd):
            if is_odd == wanted:
                yield target

    partner = {"seq": 2 * chip + other, "head": z}
    barrier = pltpu.get_barrier_semaphore()

    def tell(sem, target):
        pl.semaphore_signal(sem, inc=1, device_id=target, device_id_type=MESH)

    with jax.named_scope("greet"):
        for target in all_chips[:-1]:
            tell(barrier, {"seq": 2 * target + 1, "head": z})

        @pl.when(core == 1)
        def _():
            tell(barrier, partner)

        for plane in range(1, stacks):

            @pl.when(plane > z)
            def _():
                tell(barrier, {"seq": 2 * chip + 1, "head": plane})

    def meet_partner():
        @pl.when(core == 0)
        def _():
            pl.semaphore_wait(barrier, 1)
            tell(met, partner)

        @pl.when(core == 1)
        def _():
            pl.semaphore_wait(met, 1)

    def meet_plane():
        @pl.when(core == 1)
        def _():
            pl.semaphore_wait(barrier, 2 * (CHIPS - 1) + 2 * z)
            tell(met, partner)

        @pl.when(core == 0)
        def _():
            pl.semaphore_wait(met, 1)

    with jax.named_scope("load_rest"):
        for a in (1, 2):
            load(a, True).start()
        for a in (0, 3):
            load(a, False).start()
            load(a, True).start()
        load_gain.start()

    def remote(src, dst, send, recv, device):
        return pltpu.make_async_remote_copy(
            src_ref=src, dst_ref=dst, send_sem=send, recv_sem=recv, device_id=device, device_id_type=MESH
        )

    def to_core(src, dst, sent, received):
        return remote(src, dst, core_send.at[sent], core_recv.at[received], partner)

    def go(s, j):
        chunk, head = j // 2, j % 2
        for mine_owns in range(2):

            @pl.when((colour == head) == bool(mine_owns))
            def _():
                for target in owners(1 - mine_owns):
                    remote(
                        state.at[s, chunk, place(target, head)], gathered.at[s, chunk, chip],
                        go_send, go_recv.at[s, chunk], {"seq": 2 * target + other, "head": z},
                    ).start()

    def back(s, chunk):
        def to(target):
            remote(
                scanned.at[s, chunk, target], prefix.at[s, chunk, my_place],
                back_send, back_recv.at[s, chunk, colour], {"seq": 2 * target + other, "head": z},
            ).start()

        def twice(target):
            remote(
                scanned.at[s, chunk, target], prefix_part.at[lax.div(chip, 2)],
                twice_send, twice_recv, {"seq": 2 * target + 1, "head": z},
            ).start()

        def to_both(target):
            to(target)
            twice(target)

        def to_all(one):
            for target in all_chips[:-1]:
                pl.when(target != 0)(functools.partial(one, target))
            pl.when(chip != 0)(functools.partial(to, chip))

        if s == 0:
            for target in all_chips:
                to(target)
        elif chunk < CHUNKS - 1:
            to(0 * chip)
            to_all(to)
        else:
            owns_last = jnp.logical_and(core == 1, colour == 1)
            to(0 * chip)

            @pl.when(jnp.logical_not(owns_last))
            def _():
                to_all(to)

            @pl.when(owns_last)
            def _():
                pl.when(chip != 0)(functools.partial(twice, 0 * chip))
                to_all(to_both)
                prefix_part[lax.div(chip, 2)] = scanned[s, chunk, chip]

    def scan_back(s, chunk, reverse):
        with jax.named_scope(f"go_wait{s}{chunk}"):
            remote(gathered.at[s, chunk], gathered.at[s, chunk], go_send, go_recv.at[s, chunk], partner).wait_recv()
        with jax.named_scope(f"scan{s}{chunk}"):
            so_far = jnp.zeros((piece, HEAD_DIM), F32)
            for p in reversed(range(CHIPS)) if reverse else range(CHIPS):
                scanned[s, chunk, p] = so_far
                so_far = so_far + gathered[s, chunk, p]
        with jax.named_scope(f"back_start{s}{chunk}"):
            back(s, chunk)

    def scan_in(s, j):
        half = prefix.at[s, j // 2, pl.ds(j % 2 * (CHIPS // 2), CHIPS // 2)]
        with jax.named_scope(f"back_wait{s}{j}"):
            remote(half, half, back_send, back_recv.at[s, j // 2, j % 2], partner).wait_recv()

    def head_of(s, j):
        at = pl.ds(j % per_chunk * per_head, per_head)
        return prefix[s, j // per_chunk, at].reshape(HEAD_DIM, HEAD_DIM)

    def put_state(s, j, value):
        at = pl.ds(j % per_chunk * per_head, per_head)
        state[s, j // per_chunk, at] = value.reshape(per_head, piece, HEAD_DIM)

    def give_states(chunk):
        at = pl.ds(chunk * per_chunk, per_chunk)
        return to_core(state_out.at[at], blocks.at[core, at], 0, chunk)

    def take_states(chunk):
        at = pl.ds(chunk * per_chunk, per_chunk)
        return to_core(state_out.at[at], blocks.at[other, at], 0, chunk)

    def part_states(chunk):
        for j in heads_of(chunk):
            state_out[j] = dot(part[1, :, col(j)], part[2, :, col(j)], (0, 0))

    with jax.named_scope("load_wait"):
        for a in (1, 2):
            load(a, False).wait()
    with jax.named_scope("states_a"):
        part_states(0)
    with jax.named_scope("meet_partner"):
        meet_partner()
    give_states(0).start()
    for chunk in range(1, CHUNKS):
        part_states(chunk)
        give_states(chunk).start()
    with jax.named_scope("states_b"):
        for a in (1, 2):
            load(a, True).wait()
        for j in range(heads):
            blocks[core, j] = dot(tok[1, core, :, col(j)], tok[2, core, :, col(j)], (0, 0))
    with jax.named_scope("core_wait"):
        for chunk in range(CHUNKS):
            take_states(chunk).wait_recv()
            for j in heads_of(chunk):
                put_state(0, j, blocks[0, j] + blocks[1, j])
    with jax.named_scope("barrier"):
        meet_plane()
    with jax.named_scope("go0"):
        for j in range(heads):
            go(0, j)

    @pl.when(core == 1)
    def _():
        for plane in range(stacks - 1):

            @pl.when(plane < z)
            def _():
                tell(stack_ready, {"seq": 2 * chip, "head": plane})
                tell(stack_ready, {"seq": 2 * chip + 1, "head": plane})

    causal = lax.broadcasted_iota(jnp.int32, (tokens, tokens), 0) >= lax.broadcasted_iota(
        jnp.int32, (tokens, tokens), 1
    )

    def masked(product):
        return jnp.where(causal, product * scale, 0.0).astype(BF16)

    def gain_of(j):
        return gain[pl.ds(core * heads + j, 1), :]

    def within_block(b):
        for j in range(heads):
            w = masked(dot(tok[0, b, :, col(j)], tok[1, b, :, col(j)], (1, 1)))
            weights[b, :, col(j)] = w
            attended[b, :, col(j)] = dot(w, tok[2, b, :, col(j)], (1, 0))

    with jax.named_scope("within_own"):
        load(0, True).wait()
        load(3, True).wait()
        load_gain.wait()
        for j in range(heads):
            scaled[core, :, col(j)] = cot_own[:, col(j)].astype(F32) * gain_of(j)
        within_block(core)
    def give_tokens(n):
        return to_core(stage.at[n], came.at[n], 1, CHUNKS)

    with jax.named_scope("stage"):
        for n, a in enumerate((1, 2, 0)):
            if a == 0:
                load(0, False).wait()
            stage[n] = part[a].astype(F32)
            give_tokens(n).start()
        load(3, False).wait()
        stage[3] = cot_part[...].astype(F32)
        give_tokens(3).start()

    for chunk in range(CHUNKS):
        scan_back(0, chunk, False)

    with jax.named_scope("within_other"):
        to_core(stage, came, 1, CHUNKS).wait_recv()
        for n, a in enumerate((1, 2, 0)):
            tok[a, other] = came[n].astype(BF16)
        for j in range(heads):
            scaled[other, :, col(j)] = came[3, :, col(j)] * gain_of(j)
        within_block(other)


    squares = [jnp.zeros((tokens, HEAD_DIM), F32) for _ in range(2)]
    crosses = [jnp.zeros((tokens, HEAD_DIM), F32) for _ in range(2)]
    for head in range(heads):
        scan_in(0, head)
        with jax.named_scope(f"attended{head}"):
            for j in (head,):
                before = head_of(0, j)
                low[0, j] = before.astype(BF16)
                low[1, j] = (before + blocks[0, j]).astype(BF16)
                for b in range(2):
                    att = attended[b, :, col(j)] + scale * dot(tok[0, b, :, col(j)], low[b, j], (1, 0))
                    attended[b, :, col(j)] = att
                    squares[b] = squares[b] + att * att
                    crosses[b] = crosses[b] + att * scaled[b, :, col(j)]
    me = 2 * z + core
    with jax.named_scope("statsum"):
        for r, sums in enumerate(squares + crosses):
            stats[me, pl.ds(r, 1), :] = jnp.sum(sums.T, axis=0, keepdims=True)
        @pl.when(z < stacks - 1)
        def _():
            pl.semaphore_wait(stack_ready, stacks - 1 - z)

        for up in range(1, stacks):
            for there in (core, other):
                device = {"seq": 2 * chip + there, "head": lax.rem(z + up, stacks)}
                remote(stats.at[me], stats.at[me], stat_send, stat_recv, device).start()
        remote(stats.at[me], stats.at[me], stat_send, stat_recv, partner).start()
    rest = stats.at[pl.ds(0, 2 * stacks - 1)]
    all_stats = remote(rest, rest, stat_send, stat_recv, partner)
    with jax.named_scope("stat_wait"):
        all_stats.wait_recv()
    with jax.named_scope("stat_use"):
        total = stats[0]
        for p in range(1, 2 * stacks):
            total = total + stats[p]
        inverse_rms = lax.rsqrt(total[0:2] / width + EPSILON)
        cross_mean = total[2:4] * inverse_rms / width

        def down(row):
            return jnp.broadcast_to(row, (HEAD_DIM, tokens)).T

        inverse = [down(inverse_rms[b : b + 1]) for b in range(2)]
        cross = [down(cross_mean[b : b + 1]) for b in range(2)]
    for j in range(heads):
        with jax.named_scope(f"grads{j}"):
            sums = []
            for b in range(2):
                normed = attended[b, :, col(j)] * inverse[b]
                grad = ((scaled[b, :, col(j)] - normed * cross[b]) * inverse[b]).astype(BF16)
                grads[b, :, col(j)] = grad
                sums.append(dot(tok[0, b, :, col(j)], grad, (0, 0)))
            late[j] = sums[1]
            put_state(1, j, sums[0] + sums[1])
            go(1, j)

    def without_suffix(b):
        for j in range(heads):
            grad = grads[b, :, col(j)]
            gw = masked(dot(grad, tok[2, b, :, col(j)], (1, 1)))
            grad_f32[0, b, :, col(j)] = dot(gw, tok[1, b, :, col(j)], (1, 0)) + scale * dot(
                grad, low[b, j], (1, 1)
            )
            grad_f32[1, b, :, col(j)] = dot(gw, tok[0, b, :, col(j)], (0, 0))
            grad_f32[2, b, :, col(j)] = dot(weights[b, :, col(j)], grad, (0, 0))

    give_query = to_core(grad_f32.at[0, other], grad_came.at[0], 2, CHUNKS + 1)

    def give(n, j):
        return to_core(grad_f32.at[n, other, :, col(j)], grad_came.at[n, :, col(j)], 2, CHUNKS + 2)

    keys_values = grad_came.at[pl.ds(1, 2)]
    give_early = to_core(early, grad_came.at[pl.ds(1, 2), :, col(heads - 1)], 2, CHUNKS + 2)
    with jax.named_scope("without_suffix"):
        without_suffix(other)
        give_query.start()

        @pl.when(core == 0)
        def _():
            for n in (1, 2):
                early[n - 1] = grad_f32[n, 1, :, col(heads - 1)]
            give_early.start()

        without_suffix(core)
        result[0, :, own_cols] = grad_f32[0, core].astype(BF16)
    with jax.named_scope("dq_out"):
        give_query.wait_recv()
        result[0, :, part_cols] = grad_came[0].astype(BF16)

    for chunk in range(CHUNKS):
        scan_back(1, chunk, True)

    def with_suffix(b, j, suffix):
        grad_f32[1, b, :, col(j)] += scale * dot(tok[2, b, :, col(j)], suffix, (1, 1))
        grad_f32[2, b, :, col(j)] += scale * dot(tok[1, b, :, col(j)], suffix, (1, 0))

    for j in range(heads):
        scan_in(1, j)
        with jax.named_scope(f"with_suffix{j}"):
            after = head_of(1, j)
            with_suffix(0, j, (after + late[j]).astype(BF16))
            with_suffix(1, j, after.astype(BF16))

            @pl.when(core >= (1 if j == heads - 1 else 0))
            def _():
                for n in (1, 2):
                    give(n, j).start()

    with jax.named_scope("own_out"):
        for n in (1, 2):
            result[n, :, own_cols] = grad_f32[n, core].astype(BF16)

    with jax.named_scope("send_waits"):
        to_core(state_out, state_out, 0, 0).wait_send()
        to_core(stage, stage, 1, 0).wait_send()
        remote(state, state, go_send, go_recv.at[0, 0], partner).wait_send()
        remote(scanned, scanned, back_send, go_recv.at[0, 0], partner).wait_send()
        all_stats.wait_send()
    with jax.named_scope("final_core"):
        to_core(keys_values, keys_values, 2, CHUNKS + 2).wait_recv()

        @pl.when(core == 0)
        def _():
            for n in (1, 2):
                result[n, :, part_cols] = grad_came[n].astype(BF16)

        @pl.when(core == 1)
        def _():
            rest = (heads - 1) * HEAD_DIM
            for n in (1, 2):
                result[n, :, 0:rest] = grad_came[n, :, 0:rest].astype(BF16)
            for own in range(2):

                @pl.when(colour == own)
                def _():
                    pieces = prefix_part.at[pl.ds(0, CHIPS // 2 - own)]
                    remote(pieces, pieces, twice_send, twice_recv, partner).wait_recv()

            last = col(heads - 1)
            suffix = prefix_part[...].reshape(HEAD_DIM, HEAD_DIM).astype(BF16)
            keys = grad_came[1, :, last] + scale * dot(part[2, :, last], suffix, (1, 1))
            values = grad_came[2, :, last] + scale * dot(part[1, :, last], suffix, (1, 0))
            result[1, :, last] = keys.astype(BF16)
            result[2, :, last] = values.astype(BF16)

        to_core(grad_came, grad_came, 2, 0).wait_send()

        @pl.when(jnp.logical_and(core == 1, colour == 1))
        def _():
            pieces = scanned.at[1, 0, pl.ds(0, CHIPS - 1)]
            remote(pieces, pieces, twice_send, twice_recv, partner).wait_send()


def write_out(result, dq_hbm, dk_hbm, dv_hbm, sems):
    step = result.shape[1] // PARTS
    copies = [
        pltpu.make_async_copy(
            result.at[n, pl.ds(p * step, step)], out.at[pl.ds(p * step, step)], sems.at[PARTS * n + p]
        )
        for n, out in enumerate((dq_hbm, dk_hbm, dv_hbm))
        for p in range(PARTS)
    ]
    for copy in copies:
        copy.start()
    for copy in copies:
        copy.wait()


def per_device(stacks, queries, keys, values, cotangent, gain):
    tokens, local = queries.shape
    mine = local // 2
    heads = mine // HEAD_DIM
    piece = heads * HEAD_DIM // CHIPS // CHUNKS
    anywhere = pl.BlockSpec(memory_space=pl.ANY)
    vmem = pl.BlockSpec(memory_space=pltpu.VMEM)
    dma = pltpu.SemaphoreType.DMA
    arrays = (queries, keys, values, cotangent, gain.reshape(2 * heads, HEAD_DIM))
    result = pl.pallas_call(
        functools.partial(kernel, stacks, mine),
        out_shape=jax.ShapeDtypeStruct((3, tokens, local), BF16),
        in_specs=[pl.BlockSpec(memory_space=pltpu.HBM)] * 5,
        out_specs=vmem,
        scratch_shapes=[
            pltpu.VMEM((2 * heads, HEAD_DIM), F32),
            pltpu.VMEM((3, 2, tokens, mine), BF16),
            pltpu.VMEM((3, tokens, mine), BF16),
            pltpu.VMEM((tokens, mine), BF16),
            pltpu.VMEM((tokens, mine), BF16),
            pltpu.VMEM((4, tokens, mine), F32),
            pltpu.VMEM((4, tokens, mine), F32),
            pltpu.VMEM((2, tokens, mine), F32),
            pltpu.VMEM((2, heads, HEAD_DIM, HEAD_DIM), F32),
            pltpu.VMEM((heads, HEAD_DIM, HEAD_DIM), F32),
            pltpu.VMEM((2, CHUNKS, CHIPS, piece, HEAD_DIM), F32),
            pltpu.VMEM((2, CHUNKS, CHIPS, piece, HEAD_DIM), F32),
            pltpu.VMEM((2, CHUNKS, CHIPS, piece, HEAD_DIM), F32),
            pltpu.VMEM((2, CHUNKS, CHIPS, piece, HEAD_DIM), F32),
            pltpu.VMEM((2, heads, HEAD_DIM, HEAD_DIM), BF16),
            pltpu.VMEM((2, tokens, mine), BF16),
            pltpu.VMEM((2, tokens, mine), F32),
            pltpu.VMEM((2 * stacks, 4, tokens), F32),
            pltpu.VMEM((2, tokens, mine), BF16),
            pltpu.VMEM((heads, HEAD_DIM, HEAD_DIM), F32),
            pltpu.VMEM((3, 2, tokens, mine), F32),
            pltpu.VMEM((3, tokens, mine), F32),
            pltpu.VMEM((2, tokens, HEAD_DIM), F32),
            pltpu.VMEM((CHIPS // 2, piece, HEAD_DIM), F32),
            dma((9,)),
            dma((3,)), dma((CHUNKS + 3,)),
            dma, dma((2, CHUNKS)), dma, dma((2, CHUNKS, 2)),
            dma, dma,
            pltpu.SemaphoreType.REGULAR, pltpu.SemaphoreType.REGULAR,
            dma, dma,
        ],
        compiler_params=pltpu.CompilerParams(
            collective_id=0, has_side_effects=True, vmem_limit_bytes=24 * 1024 * 1024
        ),
        name="attention",
    )(*(pltpu.with_memory_space_constraint(a, pltpu.HBM) for a in arrays))
    out = jax.ShapeDtypeStruct((tokens, local), BF16)
    return pl.pallas_call(
        write_out,
        out_shape=(out, out, out),
        in_specs=[vmem],
        out_specs=(anywhere,) * 3,
        scratch_shapes=[dma((3 * PARTS,))],
        compiler_params=pltpu.CompilerParams(vmem_limit_bytes=4 * 1024 * 1024),
        name="write_out",
    )(result)


def solution(mesh):
    spec = P("seq", "head")
    return jax.shard_map(
        functools.partial(per_device, mesh.shape["head"]),
        mesh=mesh,
        in_specs=(spec, spec, spec, spec, P("head")),
        out_specs=(spec, spec, spec),
        check_vma=False,
    )
```

```python
import functools

import jax
import jax.numpy as jnp
from jax import lax
from jax.experimental import pallas as pl
from jax.experimental.pallas import tpu as pltpu
from jax.sharding import PartitionSpec as P

HEAD_DIM = 128
EPSILON = 1e-05
ROWS, COLUMNS = 8, 4
CHIPS = ROWS * COLUMNS
CHUNKS = 2
PARTS = 1
FIRST = (0,)
MESH = pl.DeviceIdType.MESH
F32, BF16 = jnp.float32, jnp.bfloat16


def dot(a, b, over):
    return lax.dot_general(a, b, ((over[:1], over[1:]), ((), ())), preferred_element_type=F32)


def ring_offsets(size):
    return sorted(range(size), key=lambda d: -min(d, size - d))


def kernel(
    stacks, mine,
    q_hbm, k_hbm, v_hbm, cot_hbm, gain_hbm,
    result,
    gain, tok, part, cot_own, cot_part, stage, came, scaled,
    blocks, state_out, state, gathered, scanned, prefix, low,
    weights, attended, stats, grads, late,
    grad_f32, grad_came, early, prefix_part,
    load_sem, core_send, core_recv, go_send, go_recv, back_send, back_recv, stat_send, stat_recv,
    met, stack_ready, twice_send, twice_recv,
):
    seq, z = lax.axis_index("seq"), lax.axis_index("head")
    core = lax.rem(seq, 2)
    other = 1 - core
    chip = lax.div(seq, 2)
    x, y = lax.rem(chip, COLUMNS), lax.div(chip, COLUMNS)
    heads = mine // HEAD_DIM
    per_chunk = heads // CHUNKS
    scale = HEAD_DIM ** (-0.5)
    width = 2 * mine * stacks
    tokens = tok.shape[2]
    piece = state.shape[3]
    per_head = HEAD_DIM // piece

    own_cols = pl.ds(pl.multiple_of(core * mine, mine), mine)
    part_cols = pl.ds(pl.multiple_of(other * mine, mine), mine)

    def col(j):
        return pl.ds(j * HEAD_DIM, HEAD_DIM)

    def heads_of(chunk):
        return range(chunk * per_chunk, (chunk + 1) * per_chunk)

    arrays = (q_hbm, k_hbm, v_hbm, cot_hbm)

    def load(a, own):
        if a == 3:
            target = cot_own if own else cot_part
        else:
            target = tok.at[a, core] if own else part.at[a]
        return pltpu.make_async_copy(
            arrays[a].at[:, own_cols if own else part_cols], target, load_sem.at[2 * a + int(own)]
        )

    load_gain = pltpu.make_async_copy(gain_hbm, gain, load_sem.at[8])
    with jax.named_scope("load_first"):
        for a in (1, 2):
            load(a, False).start()

    down_at = [lax.rem(y + d, ROWS) * COLUMNS for d in ring_offsets(ROWS)]
    right_at = [lax.rem(x + d, COLUMNS) for d in ring_offsets(COLUMNS)]
    offsets = [(d, r) for d in range(ROWS) for r in range(COLUMNS)]
    all_chips = [down_at[d] + right_at[r] for d, r in offsets]
    odd = [(ring_offsets(ROWS)[d] + ring_offsets(COLUMNS)[r]) % 2 for d, r in offsets]
    colour = lax.rem(x + y, 2)

    def place(target, its_colour):
        return its_colour * (CHIPS // 2) + lax.div(target, 2)

    my_place = place(chip, colour)

    def owners(wanted):
        for target, is_odd in zip(all_chips, odd):
            if is_odd == wanted:
                yield target

    partner = {"seq": 2 * chip + other, "head": z}
    barrier = pltpu.get_barrier_semaphore()

    def tell(sem, target):
        pl.semaphore_signal(sem, inc=1, device_id=target, device_id_type=MESH)

    with jax.named_scope("greet"):
        for target in all_chips[:-1]:
            tell(barrier, {"seq": 2 * target + 1, "head": z})

        @pl.when(core == 1)
        def _():
            tell(barrier, partner)

        for plane in range(1, stacks):

            @pl.when(plane > z)
            def _():
                tell(barrier, {"seq": 2 * chip + 1, "head": plane})

    def meet_partner():
        @pl.when(core == 0)
        def _():
            pl.semaphore_wait(barrier, 1)
            tell(met, partner)

        @pl.when(core == 1)
        def _():
            pl.semaphore_wait(met, 1)

    def meet_plane():
        @pl.when(core == 1)
        def _():
            pl.semaphore_wait(barrier, 2 * (CHIPS - 1) + 2 * z)
            tell(met, partner)

        @pl.when(core == 0)
        def _():
            pl.semaphore_wait(met, 1)

    with jax.named_scope("load_rest"):
        for a in (1, 2):
            load(a, True).start()
        for a in (0, 3):
            load(a, False).start()
            load(a, True).start()
        load_gain.start()

    def remote(src, dst, send, recv, device):
        return pltpu.make_async_remote_copy(
            src_ref=src, dst_ref=dst, send_sem=send, recv_sem=recv, device_id=device, device_id_type=MESH
        )

    def to_core(src, dst, sent, received):
        return remote(src, dst, core_send.at[sent], core_recv.at[received], partner)

    def go(s, j):
        chunk, head = j // 2, j % 2
        for mine_owns in range(2):

            @pl.when((colour == head) == bool(mine_owns))
            def _():
                for target in owners(1 - mine_owns):
                    remote(
                        state.at[s, chunk, place(target, head)], gathered.at[s, chunk, chip],
                        go_send, go_recv.at[s, chunk], {"seq": 2 * target + other, "head": z},
                    ).start()

    def back(s, chunk):
        def to(target):
            remote(
                scanned.at[s, chunk, target], prefix.at[s, chunk, my_place],
                back_send, back_recv.at[s, chunk, colour], {"seq": 2 * target + other, "head": z},
            ).start()

        def twice(target):
            @pl.when(jnp.logical_and(core == 1, chip != target))
            def _():
                remote(
                    scanned.at[s, chunk, target], prefix_part.at[chunk, my_place],
                    twice_send, twice_recv.at[chunk, colour], {"seq": 2 * target + 1 + 0 * chip, "head": z},
                ).start()

            @pl.when(jnp.logical_and(core == 1, chip == target))
            def _():
                prefix_part[chunk, my_place] = scanned[s, chunk, target]

        if s == 0:
            for target in all_chips:
                to(target)
        else:
            for target in FIRST:
                to(target + 0 * chip)
                twice(target)
            for target in all_chips:
                ahead = functools.reduce(jnp.logical_or, [target == t for t in FIRST])
                pl.when(jnp.logical_not(ahead))(functools.partial(to, target))

    def scan_back(s, chunk, reverse):
        with jax.named_scope(f"go_wait{s}{chunk}"):
            remote(gathered.at[s, chunk], gathered.at[s, chunk], go_send, go_recv.at[s, chunk], partner).wait_recv()
        with jax.named_scope(f"scan{s}{chunk}"):
            so_far = jnp.zeros((piece, HEAD_DIM), F32)
            for p in reversed(range(CHIPS)) if reverse else range(CHIPS):
                scanned[s, chunk, p] = so_far
                so_far = so_far + gathered[s, chunk, p]
        with jax.named_scope(f"back_start{s}{chunk}"):
            back(s, chunk)

    def scan_in(s, j):
        half = prefix.at[s, j // 2, pl.ds(j % 2 * (CHIPS // 2), CHIPS // 2)]
        with jax.named_scope(f"back_wait{s}{j}"):
            remote(half, half, back_send, back_recv.at[s, j // 2, j % 2], partner).wait_recv()

    def head_of(s, j):
        at = pl.ds(j % per_chunk * per_head, per_head)
        return prefix[s, j // per_chunk, at].reshape(HEAD_DIM, HEAD_DIM)

    def put_state(s, j, value):
        at = pl.ds(j % per_chunk * per_head, per_head)
        state[s, j // per_chunk, at] = value.reshape(per_head, piece, HEAD_DIM)

    def give_states(chunk):
        at = pl.ds(chunk * per_chunk, per_chunk)
        return to_core(state_out.at[at], blocks.at[core, at], 0, chunk)

    def take_states(chunk):
        at = pl.ds(chunk * per_chunk, per_chunk)
        return to_core(state_out.at[at], blocks.at[other, at], 0, chunk)

    def part_states(chunk):
        for j in heads_of(chunk):
            state_out[j] = dot(part[1, :, col(j)], part[2, :, col(j)], (0, 0))

    with jax.named_scope("load_wait"):
        for a in (1, 2):
            load(a, False).wait()
    with jax.named_scope("states_a"):
        part_states(0)
    with jax.named_scope("meet_partner"):
        meet_partner()
    give_states(0).start()
    for chunk in range(1, CHUNKS):
        part_states(chunk)
        give_states(chunk).start()
    with jax.named_scope("states_b"):
        for a in (1, 2):
            load(a, True).wait()
        for j in range(heads):
            blocks[core, j] = dot(tok[1, core, :, col(j)], tok[2, core, :, col(j)], (0, 0))
    with jax.named_scope("core_wait"):
        for chunk in range(CHUNKS):
            take_states(chunk).wait_recv()
            for j in heads_of(chunk):
                put_state(0, j, blocks[0, j] + blocks[1, j])
    with jax.named_scope("barrier"):
        meet_plane()
    with jax.named_scope("go0"):
        for j in range(heads):
            go(0, j)

    @pl.when(core == 1)
    def _():
        for plane in range(stacks - 1):

            @pl.when(plane < z)
            def _():
                tell(stack_ready, {"seq": 2 * chip, "head": plane})
                tell(stack_ready, {"seq": 2 * chip + 1, "head": plane})

    causal = lax.broadcasted_iota(jnp.int32, (tokens, tokens), 0) >= lax.broadcasted_iota(
        jnp.int32, (tokens, tokens), 1
    )

    def masked(product):
        return jnp.where(causal, product * scale, 0.0).astype(BF16)

    def gain_of(j):
        return gain[pl.ds(core * heads + j, 1), :]

    def within_block(b):
        for j in range(heads):
            w = masked(dot(tok[0, b, :, col(j)], tok[1, b, :, col(j)], (1, 1)))
            weights[b, :, col(j)] = w
            attended[b, :, col(j)] = dot(w, tok[2, b, :, col(j)], (1, 0))

    with jax.named_scope("within_own"):
        load(0, True).wait()
        load(3, True).wait()
        load_gain.wait()
        for j in range(heads):
            scaled[core, :, col(j)] = cot_own[:, col(j)].astype(F32) * gain_of(j)
        within_block(core)
    def give_tokens(n):
        return to_core(stage.at[n], came.at[n], 1, CHUNKS)

    with jax.named_scope("stage"):
        for n, a in enumerate((1, 2, 0)):
            if a == 0:
                load(0, False).wait()
            stage[n] = part[a].astype(F32)
            give_tokens(n).start()
        load(3, False).wait()
        stage[3] = cot_part[...].astype(F32)
        give_tokens(3).start()

    for chunk in range(CHUNKS):
        scan_back(0, chunk, False)

    with jax.named_scope("within_other"):
        to_core(stage, came, 1, CHUNKS).wait_recv()
        for n, a in enumerate((1, 2, 0)):
            tok[a, other] = came[n].astype(BF16)
        for j in range(heads):
            scaled[other, :, col(j)] = came[3, :, col(j)] * gain_of(j)
        within_block(other)


    squares = [jnp.zeros((tokens, HEAD_DIM), F32) for _ in range(2)]
    crosses = [jnp.zeros((tokens, HEAD_DIM), F32) for _ in range(2)]
    for head in range(heads):
        scan_in(0, head)
        with jax.named_scope(f"attended{head}"):
            for j in (head,):
                before = head_of(0, j)
                low[0, j] = before.astype(BF16)
                low[1, j] = (before + blocks[0, j]).astype(BF16)
                for b in range(2):
                    att = attended[b, :, col(j)] + scale * dot(tok[0, b, :, col(j)], low[b, j], (1, 0))
                    attended[b, :, col(j)] = att
                    squares[b] = squares[b] + att * att
                    crosses[b] = crosses[b] + att * scaled[b, :, col(j)]
    me = 2 * z + core
    with jax.named_scope("statsum"):
        for r, sums in enumerate(squares + crosses):
            stats[me, pl.ds(r, 1), :] = jnp.sum(sums.T, axis=0, keepdims=True)
        @pl.when(z < stacks - 1)
        def _():
            pl.semaphore_wait(stack_ready, stacks - 1 - z)

        for up in range(1, stacks):
            for there in (core, other):
                device = {"seq": 2 * chip + there, "head": lax.rem(z + up, stacks)}
                remote(stats.at[me], stats.at[me], stat_send, stat_recv, device).start()
        remote(stats.at[me], stats.at[me], stat_send, stat_recv, partner).start()
    rest = stats.at[pl.ds(0, 2 * stacks - 1)]
    all_stats = remote(rest, rest, stat_send, stat_recv, partner)
    with jax.named_scope("stat_wait"):
        all_stats.wait_recv()
    with jax.named_scope("stat_use"):
        total = stats[0]
        for p in range(1, 2 * stacks):
            total = total + stats[p]
        inverse_rms = lax.rsqrt(total[0:2] / width + EPSILON)
        cross_mean = total[2:4] * inverse_rms / width

        def down(row):
            return jnp.broadcast_to(row, (HEAD_DIM, tokens)).T

        inverse = [down(inverse_rms[b : b + 1]) for b in range(2)]
        cross = [down(cross_mean[b : b + 1]) for b in range(2)]
    for j in range(heads):
        with jax.named_scope(f"grads{j}"):
            sums = []
            for b in range(2):
                normed = attended[b, :, col(j)] * inverse[b]
                grad = ((scaled[b, :, col(j)] - normed * cross[b]) * inverse[b]).astype(BF16)
                grads[b, :, col(j)] = grad
                sums.append(dot(tok[0, b, :, col(j)], grad, (0, 0)))
            late[j] = sums[1]
            put_state(1, j, sums[0] + sums[1])
            go(1, j)

    def without_suffix(b):
        for j in range(heads):
            grad = grads[b, :, col(j)]
            gw = masked(dot(grad, tok[2, b, :, col(j)], (1, 1)))
            grad_f32[0, b, :, col(j)] = dot(gw, tok[1, b, :, col(j)], (1, 0)) + scale * dot(
                grad, low[b, j], (1, 1)
            )
            grad_f32[1, b, :, col(j)] = dot(gw, tok[0, b, :, col(j)], (0, 0))
            grad_f32[2, b, :, col(j)] = dot(weights[b, :, col(j)], grad, (0, 0))

    give_query = to_core(grad_f32.at[0, other], grad_came.at[0], 2, CHUNKS + 1)

    def give(n, j):
        return to_core(grad_f32.at[n, other, :, col(j)], grad_came.at[n, :, col(j)], 2, CHUNKS + 2)

    keys_values = grad_came.at[pl.ds(1, 2)]
    give_early = to_core(early, keys_values, 2, CHUNKS + 2)
    is_first = functools.reduce(jnp.logical_or, [chip == t for t in FIRST])
    with jax.named_scope("without_suffix"):
        without_suffix(other)
        give_query.start()

        @pl.when(jnp.logical_and(is_first, core == 0))
        def _():
            for n in (1, 2):
                early[n - 1] = grad_f32[n, 1]
            give_early.start()

        without_suffix(core)
        result[0, :, own_cols] = grad_f32[0, core].astype(BF16)
    with jax.named_scope("dq_out"):
        give_query.wait_recv()
        result[0, :, part_cols] = grad_came[0].astype(BF16)

    for chunk in range(CHUNKS):
        scan_back(1, chunk, True)

    def with_suffix(b, j, suffix):
        grad_f32[1, b, :, col(j)] += scale * dot(tok[2, b, :, col(j)], suffix, (1, 1))
        grad_f32[2, b, :, col(j)] += scale * dot(tok[1, b, :, col(j)], suffix, (1, 0))

    for j in range(heads):
        scan_in(1, j)
        with jax.named_scope(f"with_suffix{j}"):
            after = head_of(1, j)
            with_suffix(0, j, (after + late[j]).astype(BF16))
            with_suffix(1, j, after.astype(BF16))

            @pl.when(jnp.logical_not(jnp.logical_and(is_first, core == 0)))
            def _():
                for n in (1, 2):
                    give(n, j).start()

    with jax.named_scope("own_out"):
        for n in (1, 2):
            result[n, :, own_cols] = grad_f32[n, core].astype(BF16)

    with jax.named_scope("send_waits"):
        to_core(state_out, state_out, 0, 0).wait_send()
        to_core(stage, stage, 1, 0).wait_send()
        remote(state, state, go_send, go_recv.at[0, 0], partner).wait_send()
        remote(scanned, scanned, back_send, go_recv.at[0, 0], partner).wait_send()
        all_stats.wait_send()
    with jax.named_scope("final_core"):
        to_core(keys_values, keys_values, 2, CHUNKS + 2).wait_recv()

        @pl.when(jnp.logical_not(jnp.logical_and(is_first, core == 1)))
        def _():
            for n in (1, 2):
                result[n, :, part_cols] = grad_came[n].astype(BF16)

        @pl.when(jnp.logical_and(is_first, core == 1))
        def _():
            for j in range(heads):
                chunk, head = divmod(j, 2)
                for own in range(2):

                    @pl.when((colour == head) == bool(own))
                    def _():
                        pieces = prefix_part.at[chunk, pl.ds(head * (CHIPS // 2), CHIPS // 2 - own)]
                        remote(pieces, pieces, twice_send, twice_recv.at[chunk, head], partner).wait_recv()

                at = pl.ds(j % per_chunk * per_head, per_head)
                suffix = prefix_part[j // per_chunk, at].reshape(HEAD_DIM, HEAD_DIM).astype(BF16)
                cols = pl.ds(pl.multiple_of(other * mine + j * HEAD_DIM, HEAD_DIM), HEAD_DIM)
                keys = grad_came[1, :, col(j)] + scale * dot(part[2, :, col(j)], suffix, (1, 1))
                values = grad_came[2, :, col(j)] + scale * dot(part[1, :, col(j)], suffix, (1, 0))
                result[1, :, cols] = keys.astype(BF16)
                result[2, :, cols] = values.astype(BF16)

        to_core(grad_came, grad_came, 2, 0).wait_send()
        for own in range(2):
            count = CHUNKS * (len(FIRST) - own)
            if count:

                @pl.when(jnp.logical_and(core == 1, is_first == bool(own)))
                def _():
                    pieces = scanned.at[1, 0, pl.ds(0, count)]
                    remote(pieces, pieces, twice_send, twice_recv.at[0, 0], partner).wait_send()


def write_out(result, dq_hbm, dk_hbm, dv_hbm, sems):
    step = result.shape[1] // PARTS
    copies = [
        pltpu.make_async_copy(
            result.at[n, pl.ds(p * step, step)], out.at[pl.ds(p * step, step)], sems.at[PARTS * n + p]
        )
        for n, out in enumerate((dq_hbm, dk_hbm, dv_hbm))
        for p in range(PARTS)
    ]
    for copy in copies:
        copy.start()
    for copy in copies:
        copy.wait()


def per_device(stacks, queries, keys, values, cotangent, gain):
    tokens, local = queries.shape
    mine = local // 2
    heads = mine // HEAD_DIM
    piece = heads * HEAD_DIM // CHIPS // CHUNKS
    anywhere = pl.BlockSpec(memory_space=pl.ANY)
    vmem = pl.BlockSpec(memory_space=pltpu.VMEM)
    dma = pltpu.SemaphoreType.DMA
    arrays = (queries, keys, values, cotangent, gain.reshape(2 * heads, HEAD_DIM))
    result = pl.pallas_call(
        functools.partial(kernel, stacks, mine),
        out_shape=jax.ShapeDtypeStruct((3, tokens, local), BF16),
        in_specs=[pl.BlockSpec(memory_space=pltpu.HBM)] * 5,
        out_specs=vmem,
        scratch_shapes=[
            pltpu.VMEM((2 * heads, HEAD_DIM), F32),
            pltpu.VMEM((3, 2, tokens, mine), BF16),
            pltpu.VMEM((3, tokens, mine), BF16),
            pltpu.VMEM((tokens, mine), BF16),
            pltpu.VMEM((tokens, mine), BF16),
            pltpu.VMEM((4, tokens, mine), F32),
            pltpu.VMEM((4, tokens, mine), F32),
            pltpu.VMEM((2, tokens, mine), F32),
            pltpu.VMEM((2, heads, HEAD_DIM, HEAD_DIM), F32),
            pltpu.VMEM((heads, HEAD_DIM, HEAD_DIM), F32),
            pltpu.VMEM((2, CHUNKS, CHIPS, piece, HEAD_DIM), F32),
            pltpu.VMEM((2, CHUNKS, CHIPS, piece, HEAD_DIM), F32),
            pltpu.VMEM((2, CHUNKS, CHIPS, piece, HEAD_DIM), F32),
            pltpu.VMEM((2, CHUNKS, CHIPS, piece, HEAD_DIM), F32),
            pltpu.VMEM((2, heads, HEAD_DIM, HEAD_DIM), BF16),
            pltpu.VMEM((2, tokens, mine), BF16),
            pltpu.VMEM((2, tokens, mine), F32),
            pltpu.VMEM((2 * stacks, 4, tokens), F32),
            pltpu.VMEM((2, tokens, mine), BF16),
            pltpu.VMEM((heads, HEAD_DIM, HEAD_DIM), F32),
            pltpu.VMEM((3, 2, tokens, mine), F32),
            pltpu.VMEM((3, tokens, mine), F32),
            pltpu.VMEM((2, tokens, mine), F32),
            pltpu.VMEM((CHUNKS, CHIPS, piece, HEAD_DIM), F32),
            dma((9,)),
            dma((3,)), dma((CHUNKS + 3,)),
            dma, dma((2, CHUNKS)), dma, dma((2, CHUNKS, 2)),
            dma, dma,
            pltpu.SemaphoreType.REGULAR, pltpu.SemaphoreType.REGULAR,
            dma, dma((CHUNKS, 2)),
        ],
        compiler_params=pltpu.CompilerParams(
            collective_id=0, has_side_effects=True, vmem_limit_bytes=24 * 1024 * 1024
        ),
        name="attention",
    )(*(pltpu.with_memory_space_constraint(a, pltpu.HBM) for a in arrays))
    out = jax.ShapeDtypeStruct((tokens, local), BF16)
    return pl.pallas_call(
        write_out,
        out_shape=(out, out, out),
        in_specs=[vmem],
        out_specs=(anywhere,) * 3,
        scratch_shapes=[dma((3 * PARTS,))],
        compiler_params=pltpu.CompilerParams(vmem_limit_bytes=4 * 1024 * 1024),
        name="write_out",
    )(result)


def solution(mesh):
    spec = P("seq", "head")
    return jax.shard_map(
        functools.partial(per_device, mesh.shape["head"]),
        mesh=mesh,
        in_specs=(spec, spec, spec, spec, P("head")),
        out_specs=(spec, spec, spec),
        check_vma=False,
    )
```
